256 devices in a mesh: ctx: 32 (over x, y, core), tp: 8 (over z).
Axes of the slice: x: 4, y: 4, z: 8, core: 2. Of those that a mesh axis runs over, the one named last changes fastest.
Arguments:
- patches: bfloat16 [16384, 1280], P('ctx'), may hold values from -21 to 21
- window_ids: int32 [16384], P('ctx'), may hold values from -1 to 4095, as said below
- positions: int32 [4096], P('ctx'), may hold values from 0 to 32768, as said below
- text_embed: bfloat16 [32768, 8192], P('ctx', 'tp'), may hold values from -6 to 6
- cotangent: bfloat16 [32768, 8192], P('ctx', 'tp'), may hold values from -0.119628906 to 0.119628906
- qkv_weight: bfloat16 [3, 1280, 1280], P(None, None, 'tp'), may hold values from -0.15625 to 0.15625
- out_weight: bfloat16 [1280, 1280], P('tp'), may hold values from -0.15625 to 0.15625
- merger_weight: bfloat16 [5120, 8192], P('ctx', 'tp'), may hold values from -0.078125 to 0.078125
- norm_gain: bfloat16 [8192], P('tp'), may hold values from 0.099609375 to 1.8984375
Outputs:
- normed: bfloat16 [32768, 8192], P('ctx', 'tp')
- merger_grad: float32 [5120, 8192], P('ctx', 'tp')
The draws below stay inside these ranges and needn't reach their ends.
Inputs may be any that keep to these rules, and one draw needn't show every extreme that they name: `window_ids`: windows are runs of consecutive patch slots of one index of ctx, each of 4 to 64 slots and a multiple of 4; every window id belongs to one index of ctx; the padding slots of an index of ctx come after its live slots and carry -1. Merged slot j of an index of ctx covers its patch slots 4j to 4j+3 and is live exactly when those are; live slots carry distinct positions, dead ones carry 32768. The live slots of one index of ctx name at most 4 positions among the 1024 positions of any one index of ctx.
All inputs are finite; a program needn't handle non-finite values.
Results may differ from the reference program's by a relative error of at most 0.014.
Values may be sent and summed in bfloat16 or wider, within the bound.
A program may use at most 128 MiB of HBM per device.

```python
import jax
import jax.numpy as jnp
from jax import lax

DV = 1280
HEADS = 16
D = 8192
V_DEV = 512
TOK_DEV = 1024
HEAD_DIM = 80
MERGE_IN = 5120
M_DEV = 128
CAP = 4
TOKENS = 32768
N_CTX = 32


def layout(key):
    base = jax.random.fold_in(key, 7)
    keys = jax.random.split(base, 7)
    live = jnp.minimum(jax.random.randint(keys[0], (N_CTX,), M_DEV // 8, M_DEV + 1), jax.random.randint(keys[1], (N_CTX,), M_DEV // 8, M_DEV + 1))
    full_device = jax.random.randint(keys[2], (), 0, N_CTX)
    live = jnp.where(jnp.arange(N_CTX) == full_device, M_DEV, live)
    busiest = jax.random.randint(keys[3], (), 0, N_CTX)
    rest = jax.vmap(lambda k: jax.random.permutation(k, N_CTX - 1))(jax.random.split(keys[4], N_CTX))
    spread = jnp.concatenate([jnp.zeros((N_CTX, 1), jnp.int32), 1 + rest.astype(jnp.int32)], axis=1)
    row_order = jax.vmap(lambda k: jax.random.permutation(k, TOK_DEV))(jax.random.split(keys[5], N_CTX)).astype(jnp.int32)
    source = jnp.arange(N_CTX, dtype=jnp.int32)[:, None]
    slot = jnp.arange(M_DEV, dtype=jnp.int32)[None, :]
    group = slot // CAP
    within = slot % CAP
    target = (busiest + jnp.take_along_axis(spread, jnp.broadcast_to(group, (N_CTX, M_DEV)), axis=1)) % N_CTX
    local_row = row_order[target, source * CAP + within]
    alive = slot < live[:, None]
    positions = jnp.where(alive, target * TOK_DEV + local_row, TOKENS).reshape(-1).astype(jnp.int32)
    lengths = jax.random.randint(keys[6], (N_CTX, M_DEV), 1, 17)
    ends = jnp.cumsum(lengths, axis=1)
    window_of_unit = jnp.sum((ends[:, None, :] <= slot[:, :, None]).astype(jnp.int32), axis=2)
    unit_ids = jnp.where(alive, source * M_DEV + window_of_unit, -1)
    window_ids = jnp.repeat(unit_ids, 4, axis=1).reshape(-1).astype(jnp.int32)
    return (window_ids, positions)


def draw_window_ids(key, part):
    return layout(key)[0]


def draw_positions(key, part):
    return layout(key)[1]


def draw_patches(key, part):
    base = jax.random.fold_in(key, 11)
    keys = jax.random.split(base, 1)
    values = jnp.clip(jax.random.normal(keys[0], (N_CTX * V_DEV, DV), jnp.float32), -6.0, 6.0)
    return values.astype(jnp.bfloat16)


def block_scale(rng, extent, cuts, smallest, high):
    level = 1.0
    for position, shards_of in cuts:
        draws = jax.random.uniform(jax.random.fold_in(jax.random.fold_in(rng, 6), position), (shards_of,), jnp.float32, smallest / len(cuts), high / len(cuts))
        level = level * jnp.repeat(jnp.exp(draws), extent[position] // shards_of).reshape((-1,) + (1,) * (len(extent) - 1 - position))
    return level


def scatter_about(key, dims, deviation, limit, cuts=(), held_as=jnp.bfloat16):
    result = jax.random.normal(key, dims, jnp.float32) * deviation
    if len(cuts) > 0:
        result = block_scale(key, dims, cuts, -0.22, 0.18) * result
    return jnp.clip(result, min=-limit, max=limit).astype(held_as)


def setup_inputs(seed: int = 0) -> dict:
    splits = jax.random.split(jax.random.key(seed), 10)
    patches = draw_patches(jax.random.fold_in(splits[9], 71), 0)
    window_ids = draw_window_ids(jax.random.fold_in(splits[9], 71), 0)
    positions = draw_positions(jax.random.fold_in(splits[9], 71), 0)
    text_embed = scatter_about(splits[3], (TOKENS, D), 1.0, 6.0, ((0, 32), (1, 8)))
    cotangent = scatter_about(splits[4], (TOKENS, D), 0.02, 0.119628906, ((0, 32), (1, 8)))
    qkv_weight = scatter_about(splits[5], (3, DV, DV), DV ** -0.5, 0.15625, ((2, 8),))
    out_weight = scatter_about(splits[6], (DV, DV), DV ** -0.5, 0.15625, ((0, 8),))
    merger_weight = scatter_about(splits[7], (MERGE_IN, D), MERGE_IN ** -0.5, 0.078125, ((0, 32), (1, 8)))
    norm_gain = jnp.clip(1.0 + 0.18 * jax.random.normal(splits[8], (D,), jnp.float32), 0.099609375, 1.8984375).astype(jnp.bfloat16)
    return dict(patches=patches, window_ids=window_ids, positions=positions, text_embed=text_embed, cotangent=cotangent, qkv_weight=qkv_weight, out_weight=out_weight, merger_weight=merger_weight, norm_gain=norm_gain)


def attend(block_x, block_ids, qkv_weight, out_weight):
    projected = [jnp.dot(block_x, qkv_weight[i], preferred_element_type=jnp.float32).astype(jnp.bfloat16) for i in range(3)]
    queries = projected[0].reshape(V_DEV, HEADS, HEAD_DIM)
    keys_all = projected[1].reshape(V_DEV, HEADS, HEAD_DIM)
    values = projected[2].reshape(V_DEV, HEADS, HEAD_DIM)
    width = min(512, V_DEV)
    factor = 1.0 / HEAD_DIM ** 0.5

    def one_block(block_index):
        first_row = block_index * width
        query_rows = lax.dynamic_slice_in_dim(queries, first_row, width, 0)
        query_ids = lax.dynamic_slice_in_dim(block_ids, first_row, width, 0)
        scores = jnp.einsum('qhd,khd->hqk', query_rows.astype(jnp.float32), keys_all.astype(jnp.float32)) * factor
        allowed = (query_ids[:, None] == block_ids[None, :]) & (block_ids[None, :] >= 0)
        scores = jnp.where(allowed[None], scores, jnp.float32(-1e+30))
        highest = lax.optimization_barrier(jnp.max(scores, axis=2, keepdims=True))
        weights = jnp.exp(scores - highest)
        probs = (weights / lax.optimization_barrier(jnp.sum(weights, axis=2, keepdims=True))).astype(jnp.bfloat16)
        attended = jnp.einsum('hqk,khd->qhd', probs.astype(jnp.float32), values.astype(jnp.float32))
        return attended.astype(jnp.bfloat16).reshape(width, DV)
    attended = lax.map(one_block, jnp.arange(V_DEV // width, dtype=jnp.int32)).reshape(V_DEV, DV)
    output = jnp.dot(attended, out_weight, preferred_element_type=jnp.float32)
    return (block_x.astype(jnp.float32) + output).astype(jnp.bfloat16)

def norm_rows(rows_x, rows_cot, gain):
    values = rows_x.astype(jnp.float32)
    gained = gain.astype(jnp.float32)[None, :] * rows_cot.astype(jnp.float32)
    squares = lax.optimization_barrier(jnp.sum(values * values, axis=1))
    inner = lax.optimization_barrier(jnp.sum(values * gained, axis=1))
    scale = lax.rsqrt(squares / D + 1e-06)[:, None]
    normed = (values * scale * gain.astype(jnp.float32)[None, :]).astype(jnp.bfloat16)
    d_embed = (scale * gained - values * scale ** 3 * inner[:, None] / D).astype(jnp.bfloat16)
    return (normed, d_embed)

def reference(patches, window_ids, positions, text_embed, cotangent, qkv_weight, out_weight, merger_weight, norm_gain):
    grouped = patches.reshape(N_CTX, V_DEV, DV)
    grouped_ids = window_ids.reshape(N_CTX, V_DEV)
    hidden = lax.map(lambda pair: attend(pair[0], pair[1], qkv_weight, out_weight), (grouped, grouped_ids))
    merged_in = hidden.reshape(N_CTX * M_DEV, MERGE_IN)
    merged = jnp.dot(merged_in, merger_weight, preferred_element_type=jnp.float32).astype(jnp.bfloat16)
    embedded = text_embed.at[positions].set(merged, mode='drop')
    normed, d_embed = lax.map(lambda pair: norm_rows(pair[0], pair[1], norm_gain), (embedded.reshape(N_CTX, TOK_DEV, D), cotangent.reshape(N_CTX, TOK_DEV, D)))
    normed = normed.reshape(TOKENS, D)
    d_embed = d_embed.reshape(TOKENS, D)
    d_merged = jnp.take(d_embed, positions, axis=0, mode='fill', fill_value=0)
    merger_grad = jnp.dot(merged_in.T, d_merged, preferred_element_type=jnp.float32)
    return (normed, merger_grad)
```

```python
import jax
import jax.numpy as jnp
from jax import lax
from jax.experimental import pallas as pl
from jax.experimental.pallas import tpu as pltpu
from jax.sharding import PartitionSpec as P

MESH = pl.DeviceIdType.MESH
D = 8192
HEAD_DIM = 80
NX, NY, NC, NZ = 4, 4, 2, 8
N_CTX = 32
SLOTS = 128
TOK = 1024
DV = 1280
HCOLS = 160
ROWS_W = 160
F32 = jnp.float32
BF16 = jnp.bfloat16


def remote(src, dst, send, recv, dev):
    return pltpu.make_async_remote_copy(
        src_ref=src, dst_ref=dst, send_sem=send, recv_sem=recv, device_id=dev, device_id_type=MESH
    )


def dot(a, b):
    return jnp.dot(a, b, preferred_element_type=F32)


def dot_nt(a, b):
    return lax.dot_general(a, b, (((1,), (1,)), ((), ())), preferred_element_type=F32)


def iota(shape, dim):
    return lax.broadcasted_iota(jnp.int32, shape, dim)


class Place:
    def __init__(self):
        self.ctx = lax.axis_index("ctx")
        self.z = lax.axis_index("tp")
        self.core = self.ctx % 2
        y = (self.ctx // 2) % NY
        x = self.ctx // (2 * NY)
        self.f = x * (1 - self.core) + y * self.core
        self.g = y * (1 - self.core) + x * self.core
        self.sib = self.ctx + 1 - 2 * self.core
        self.offs = (0, 3, 1, 2)

    def ctx_of(self, f, g):
        x = f * (1 - self.core) + g * self.core
        y = g * (1 - self.core) + f * self.core
        return (x * NY + y) * 2 + self.core

    def near(self, df, dg):
        return self.ctx_of((self.f + df) % 4, (self.g + dg) % 4)

    def dev(self, df, dg):
        return {"ctx": self.near(df, dg), "tp": self.z}


class PlaneGather:
    def __init__(self, place, buf, rows, ss, rs):
        self.p, self.buf, self.rows, self.half = place, buf, rows, rows // 2
        self.ss, self.rs = ss, rs
        self.started = []

    def block(self, df, dg, part=None):
        base = self.p.near(df, dg) * self.rows
        if part is None:
            return self.buf.at[pl.ds(pl.multiple_of(base, 32), self.rows), :]
        base = base + part * self.half
        return self.buf.at[pl.ds(pl.multiple_of(base, 16), self.half), :]

    def send(self, n, region, dev):
        c = remote(region, region, self.ss.at[n], self.rs.at[n], dev)
        c.start()
        self.started.append(c)

    def recv(self, n, region):
        remote(region, region, self.ss.at[n], self.rs.at[n], self.p.dev(0, 1)).wait_recv()

    def sibling(self, i, j):
        o = self.p.offs
        self.send(20 + 4 * i + j, self.block(o[i], o[j]), {"ctx": self.p.sib, "tp": self.p.z})

    def item(self, i):
        o = self.p.offs
        self.send(4 + 4 * i, self.block(o[i], 0), self.p.dev(0, 1))
        self.send(5 + 4 * i, self.block(o[i], 0), self.p.dev(0, 3))
        self.sibling(i, 0)

    def start(self):
        own = self.block(0, 0)
        self.send(0, own, self.p.dev(1, 0))
        self.send(1, own, self.p.dev(3, 0))
        self.item(0)

    def first(self):
        self.recv(0, self.block(3, 0))
        self.send(2, self.block(3, 0, 0), self.p.dev(1, 0))
        self.item(1)
        self.recv(1, self.block(1, 0))
        self.send(3, self.block(1, 0, 1), self.p.dev(3, 0))
        self.item(2)

    def second(self):
        self.recv(2, self.block(2, 0, 0))
        self.recv(3, self.block(2, 0, 1))
        self.item(3)

    def third(self, i):
        o = self.p.offs[i]
        self.recv(4 + 4 * i, self.block(o, 3))
        self.send(6 + 4 * i, self.block(o, 3, 0), self.p.dev(0, 1))
        self.sibling(i, 1)
        self.recv(5 + 4 * i, self.block(o, 1))
        self.send(7 + 4 * i, self.block(o, 1, 1), self.p.dev(0, 3))
        self.sibling(i, 2)

    def fourth(self, i):
        o = self.p.offs[i]
        self.recv(6 + 4 * i, self.block(o, 2, 0))
        self.recv(7 + 4 * i, self.block(o, 2, 1))
        self.sibling(i, 3)

    def from_sibling(self, i, j):
        o = self.p.offs
        base = self.p.near(o[i], o[j]) + 1 - 2 * self.p.core
        region = self.buf.at[pl.ds(pl.multiple_of(base * self.rows, 32), self.rows), :]
        self.recv(20 + 4 * j + i, region)

    def pair_rows(self, i, j):
        o = self.p.offs
        return (self.p.near(o[i], o[j]) - self.p.core) * self.rows

    def finish(self):
        for c in self.started:
            c.wait_send()


class Ring:
    def __init__(self, place, region, ss, rs):
        self.p, self.region, self.ss, self.rs = place, region, ss, rs
        self.started = []

    def step(self, s):
        z = self.p.z
        for way in range(2):
            sign = 1 - 2 * way
            part = way if s == 4 else None
            src = self.region((z - sign * (s - 1) + NZ) % NZ, part)
            c = remote(
                src, src, self.ss.at[4 * way + s - 1], self.rs.at[4 * way + s - 1],
                {"ctx": self.p.ctx, "tp": (z + sign + NZ) % NZ},
            )
            c.start()
            self.started.append(c)

    def recv(self, s):
        z = self.p.z
        for way in range(2):
            sign = 1 - 2 * way
            part = way if s == 4 else None
            dst = self.region((z - sign * s + NZ) % NZ, part)
            remote(
                dst, dst, self.ss.at[4 * way + s - 1], self.rs.at[4 * way + s - 1],
                {"ctx": self.p.ctx, "tp": (z + sign + NZ) % NZ},
            ).wait_recv()

    def finish(self):
        for c in self.started:
            c.wait_send()


def kernel(
    pat, wid, pos, text_in, cot_in, qkv, ow_in, w_in, gain,
    normed_out, grad_out,
    wf, gf, owf, attf, att_t, hid, perm, colsend, colin, colf, colg, cols, text, cot, normed,
    q0s, q1s, ks, vts, widc, mrow, rows_send, rows_in, incf, idx_send, idx_in, stats, cotsel, scol, drow,
    local, w_ss, w_rs, g_ss, g_rs, ow_ss, ow_rs, osib_ss, osib_rs, at_ss, at_rs,
    ix_ss, ix_rs, rw_ss, rw_rs, co_ss, co_rs, st_ss, st_rs,
):
    p = Place()
    ctx, z, core = p.ctx, p.z, p.core

    def other(d):
        return (ctx + d) % N_CTX

    def behind(d):
        return (ctx + N_CTX - d) % N_CTX

    barrier = pltpu.get_barrier_semaphore()

    @pl.loop(1, N_CTX)
    def _(d):
        pl.semaphore_signal(barrier, inc=1, device_id={"ctx": other(d), "tp": z}, device_id_type=MESH)

    @pl.loop(1, NZ)
    def _(d):
        pl.semaphore_signal(barrier, inc=1, device_id={"ctx": ctx, "tp": (z + d) % NZ}, device_id_type=MESH)

    own_w = wf.at[pl.ds(pl.multiple_of(ctx * ROWS_W, 32), ROWS_W), :]
    own_ow = owf.at[pl.ds(pl.multiple_of(z * HCOLS, 32), HCOLS), :]
    load_w = pltpu.make_async_copy(w_in, own_w, local.at[0])
    load_ow = pltpu.make_async_copy(ow_in, own_ow, local.at[1])
    load_text = pltpu.make_async_copy(text_in, text, local.at[2])
    load_cot = pltpu.make_async_copy(cot_in, cot, local.at[3])
    load_w.start()
    load_ow.start()
    load_text.start()
    load_cot.start()

    pos_row = pos[...]
    pos_col = jnp.broadcast_to(pos_row, (SLOTS, SLOTS)).T
    t_row = pos_row // TOK
    t_col = pos_col // TOK
    same = t_col == t_row
    earlier_down = same & (iota((SLOTS, SLOTS), 0) < iota((SLOTS, SLOTS), 1))
    earlier_across = same & (iota((SLOTS, SLOTS), 1) < iota((SLOTS, SLOTS), 0))
    rank_row = jnp.sum(jnp.where(earlier_down, 1.0, 0.0).astype(F32), axis=0, keepdims=True)
    rank_col = jnp.sum(jnp.where(earlier_across, 1.0, 0.0).astype(F32), axis=1, keepdims=True)
    live_row = t_row < N_CTX
    bucket_row = jnp.where(live_row, t_row.astype(F32) * 4.0 + rank_row, -1.0)
    to_owner = jnp.where(iota((N_CTX, SLOTS), 0) == t_row, 1.0, 0.0).astype(BF16)
    row_no = pos_col % TOK + 1
    lane_of = rank_col.astype(jnp.int32) * N_CTX + ctx
    at_lane = lane_of == iota((SLOTS, SLOTS), 1)
    high = jnp.where(at_lane, (row_no // 32).astype(F32), 0.0).astype(BF16)
    low = jnp.where(at_lane, (row_no % 32).astype(F32), 0.0).astype(BF16)
    index_rows = (dot(to_owner, high) * 32.0 + dot(to_owner, low)).astype(jnp.int32)
    for t in range(N_CTX):
        idx_send[t] = jnp.broadcast_to(index_rows[t : t + 1, :], (8, SLOTS))
    idx_in[ctx] = idx_send[ctx]

    for b in range(4):
        widc[128 * b : 128 * (b + 1), :] = jnp.broadcast_to(wid[:, 128 * b : 128 * (b + 1)], (128, 128)).T

    pl.semaphore_wait(barrier, N_CTX - 1 + NZ - 1)

    wg = PlaneGather(p, wf, ROWS_W, w_ss, w_rs)
    load_w.wait()
    wg.start()

    def ow_region(zz, part):
        base = pl.multiple_of(zz * HCOLS + core * 80, 16)
        if part is None:
            return owf.at[pl.ds(base, 80), :]
        return owf.at[pl.ds(base, 80), pl.ds(part * 640, 640)]

    def att_region(zz, part):
        if part is None:
            return attf.at[pl.ds(pl.multiple_of(zz * HCOLS, 32), HCOLS), :]
        return attf.at[pl.ds(pl.multiple_of(zz * HCOLS + part * 80, 16), 80), :]

    osib = []

    def ow_to_sibling(k, zz):
        src = ow_region(zz, None)
        c = remote(src, src, osib_ss.at[k], osib_rs.at[k], {"ctx": p.sib, "tp": z})
        c.start()
        osib.append(c)

    og = Ring(p, ow_region, ow_ss, ow_rs)
    ag = Ring(p, att_region, at_ss, at_rs)
    load_ow.wait()
    og.step(1)

    @pl.loop(1, N_CTX)
    def _(d):
        remote(
            idx_send.at[other(d)], idx_in.at[ctx], ix_ss.at[d], ix_rs.at[d], {"ctx": other(d), "tp": z}
        ).start()

    patches = pat[...]
    lane = iota((512, HCOLS), 1)
    q = dot(patches, qkv[0]).astype(BF16).astype(F32)
    q0s[...] = jnp.where(lane < HEAD_DIM, q, 0.0).astype(BF16)
    q1s[...] = jnp.where(lane < HEAD_DIM, 0.0, q).astype(BF16)
    ks[...] = dot(patches, qkv[1]).astype(BF16)
    vts[...] = dot(patches, qkv[2]).astype(BF16).T
    wg.first()

    factor = 1.0 / HEAD_DIM**0.5

    @pl.loop(0, 4)
    def _(b):
        cols_b = pl.ds(pl.multiple_of(b * 128, 128), 128)
        ids = wid[:, cols_b]
        allowed = (widc[...] == ids) & (widc[...] >= 0)
        parts = []
        for qs in (q0s, q1s):
            scores = dot_nt(ks[...], qs[cols_b, :]) * factor
            scores = jnp.where(allowed, scores, -1e30)
            weights = jnp.exp(scores - jnp.max(scores, axis=0, keepdims=True))
            probs = (weights / jnp.sum(weights, axis=0, keepdims=True)).astype(BF16)
            parts.append(dot(vts[...], probs))
        row = iota((HCOLS, 128), 0)
        attf[pl.ds(pl.multiple_of(z * HCOLS, 32), HCOLS), cols_b] = jnp.where(
            row < HEAD_DIM, parts[0], parts[1]
        ).astype(BF16)

    ag.step(1)

    wg.second()
    og.recv(1)
    og.step(2)
    wg.third(0)
    ag.recv(1)
    ag.step(2)
    og.recv(2)
    og.step(3)
    wg.third(1)
    wg.third(2)
    ag.recv(2)
    ag.step(3)
    og.recv(3)
    og.step(4)
    wg.third(3)
    ag.recv(3)
    ag.step(4)
    for k in (0, 1, 2, 4, 5, 6):
        ow_to_sibling(k, (z + 5 + k) % NZ)
    for i in range(4):
        wg.fourth(i)
    og.recv(4)
    ow_to_sibling(7, (z + 4) % NZ)
    ag.recv(4)
    for k in (0, 1, 2, 4, 5, 6, 7):
        zz = (z + 5 + k) % NZ if k < 7 else (z + 4) % NZ
        dst = owf.at[pl.ds(pl.multiple_of(zz * HCOLS + (1 - core) * 80, 16), 80), :]
        remote(dst, dst, osib_ss.at[k], osib_rs.at[k], {"ctx": p.sib, "tp": z}).wait_recv()

    for zz in range(NZ):
        att_t[:, zz * HCOLS : (zz + 1) * HCOLS] = attf[zz * HCOLS : (zz + 1) * HCOLS, :].T

    @pl.loop(0, 5)
    def _(n):
        cols_n = pl.ds(pl.multiple_of(n * 256, 256), 256)
        out = dot(att_t[...], owf[:, cols_n])
        hid[:, cols_n] = (pat[:, cols_n].astype(F32) + out).astype(BF16)

    spread_at = jnp.where(iota((SLOTS, 512), 0) == iota((SLOTS, 512), 1) // 4, 1.0, 0.0).astype(BF16)
    bucket512 = dot(jnp.broadcast_to(bucket_row, (8, SLOTS)).astype(BF16), spread_at)[0:1, :]
    chosen = iota((SLOTS, 512), 0).astype(F32) == bucket512
    for i in range(4):
        select = jnp.where(chosen & (iota((SLOTS, 512), 1) % 4 == i), 1.0, 0.0).astype(BF16)
        for n in range(5):
            perm[:, i * DV + n * 256 : i * DV + (n + 1) * 256] = dot(
                select, hid[:, n * 256 : (n + 1) * 256]
            ).astype(BF16)

    for i in range(4):
        for j in range(4):
            wg.from_sibling(i, j)

    @pl.loop(0, 4)
    def _(n):
        cols_n = pl.ds(pl.multiple_of(n * 256, 256), 256)
        mrow[:, cols_n] = dot(perm[...], wf[:, cols_n]).astype(BF16).astype(F32)

    @pl.loop(0, N_CTX // 2)
    def _(t):
        eight = mrow[pl.ds(pl.multiple_of(t * 8, 8), 8), :]
        rows_send[2 * t] = eight[0:4, :].astype(BF16)
        rows_send[2 * t + 1] = eight[4:8, :].astype(BF16)

    @pl.loop(1, N_CTX)
    def _(d):
        remote(
            rows_send.at[other(d)], rows_in.at[ctx], rw_ss.at[d], rw_rs.at[d], {"ctx": other(d), "tp": z}
        ).start()

    rows_in[ctx] = rows_send[ctx]

    for n in range(40):
        colsend[n * 128 : (n + 1) * 128, :] = perm[:, n * 128 : (n + 1) * 128].T

    def col_block(c):
        return colsend.at[pl.ds(pl.multiple_of(c * ROWS_W, 32), ROWS_W), :]

    @pl.loop(1, N_CTX)
    def _(d):
        remote(
            col_block(other(d)), colin.at[ctx], co_ss.at[d], co_rs.at[d], {"ctx": other(d), "tp": z}
        ).start()

    colin[ctx] = colsend[pl.ds(pl.multiple_of(ctx * ROWS_W, 32), ROWS_W), :]

    @pl.loop(1, N_CTX)
    def _(d):
        remote(
            idx_send.at[other(d)], idx_in.at[behind(d)], ix_ss.at[d], ix_rs.at[d], {"ctx": other(d), "tp": z}
        ).wait()

    load_text.wait()
    load_cot.wait()
    at_row = (jnp.sum(idx_in[...], axis=0) - 1)[0:1, :]
    at_col = jnp.broadcast_to(at_row, (SLOTS, SLOTS)).T
    for b in range(8):
        drow[:, 128 * b : 128 * (b + 1)] = jnp.where(
            at_col == iota((SLOTS, SLOTS), 1) + 128 * b, 1.0, 0.0
        ).astype(BF16)

    @pl.loop(0, 4)
    def _(n):
        cols_n = pl.ds(pl.multiple_of(n * 256, 256), 256)
        cotsel[:, cols_n] = dot(drow[...], cot[:, cols_n])

    @pl.loop(1, N_CTX)
    def _(d):
        remote(
            rows_send.at[other(d)], rows_in.at[behind(d)], rw_ss.at[d], rw_rs.at[d], {"ctx": other(d), "tp": z}
        ).wait()

    @pl.loop(0, N_CTX)
    def _(s):
        four = rows_in[s].astype(F32)
        for k in range(4):
            incf[pl.ds(k * N_CTX + s, 1), :] = four[k : k + 1, :]

    gain_row = gain[...].astype(F32)

    @pl.loop(0, 8)
    def _(b):
        rows_b = pl.ds(pl.multiple_of(b * 128, 128), 128)
        placed = jnp.where(iota((128, SLOTS), 0) + 128 * b == at_row, 1.0, 0.0).astype(F32)
        taken = jnp.sum(placed, axis=1, keepdims=True) > 0.0
        vision = dot(placed.astype(BF16), incf[...].astype(BF16))
        sq = jnp.zeros((128, 128), F32)
        inner = jnp.zeros((128, 128), F32)
        for n in range(8):
            cols_n = slice(128 * n, 128 * (n + 1))
            emb = jnp.where(taken, vision[:, cols_n], text[rows_b, cols_n].astype(F32))
            text[rows_b, cols_n] = emb.astype(BF16)
            sq = sq + emb * emb
            inner = inner + emb * (gain_row[:, cols_n] * cot[rows_b, cols_n].astype(F32))
        stats[z, pl.ds(b, 1), :] = jnp.sum(sq.T, axis=0, keepdims=True)
        stats[z, pl.ds(8 + b, 1), :] = jnp.sum(inner.T, axis=0, keepdims=True)

    def stat_copy(d, slot):
        return remote(
            stats.at[z], stats.at[slot], st_ss.at[d], st_rs.at[d], {"ctx": ctx, "tp": (z + d) % NZ}
        )

    @pl.loop(1, NZ)
    def _(d):
        stat_copy(d, z).start()

    @pl.loop(1, N_CTX)
    def _(d):
        remote(
            col_block(other(d)), colin.at[behind(d)], co_ss.at[d], co_rs.at[d], {"ctx": other(d), "tp": z}
        ).wait()

    @pl.loop(0, N_CTX)
    def _(s):
        rows_s = pl.ds(pl.multiple_of(s * SLOTS, 128), SLOTS)
        came = colin[s].astype(F32)
        colf[rows_s, :] = came[0:128, :].T
        colg[rows_s, :] = jnp.concatenate([came[128:160, :], jnp.zeros((96, 128), F32)], axis=0).T

    @pl.loop(1, NZ)
    def _(d):
        stat_copy(d, (z + NZ - d) % NZ).wait()

    total = jnp.sum(stats[...], axis=0)
    scale = lax.rsqrt(total[0:8, :] / D + 1e-06)
    inner_all = total[8:16, :]
    scale_at = jnp.zeros((1, SLOTS), F32)
    inner_at = jnp.zeros((1, SLOTS), F32)
    for b in range(8):
        here = iota((128, SLOTS), 0) + 128 * b == at_row
        scale_b = jnp.broadcast_to(scale[b : b + 1, :], (128, 128)).T
        inner_b = jnp.broadcast_to(inner_all[b : b + 1, :], (128, 128)).T
        scol[128 * b : 128 * (b + 1), :] = scale_b
        scale_at = scale_at + jnp.sum(jnp.where(here, scale_b, 0.0), axis=0, keepdims=True)
        inner_at = inner_at + jnp.sum(jnp.where(here, inner_b, 0.0), axis=0, keepdims=True)
    s_at = jnp.broadcast_to(scale_at, (SLOTS, SLOTS)).T
    i_at = jnp.broadcast_to(inner_at, (SLOTS, SLOTS)).T
    own_g = pl.ds(pl.multiple_of(ctx * SLOTS, 128), SLOTS)
    for n in range(8):
        cols_n = slice(128 * n, 128 * (n + 1))
        gained = gain_row[:, cols_n] * cotsel[:, cols_n]
        gf[own_g, cols_n] = (s_at * gained - incf[:, cols_n] * (s_at * s_at * s_at) * i_at / D).astype(BF16)

    gg = PlaneGather(p, gf, SLOTS, g_ss, g_rs)
    gg.start()

    def normed_copy(b):
        rows_b = pl.ds(pl.multiple_of(b * 256, 256), 256)
        return pltpu.make_async_copy(normed.at[rows_b, :], normed_out.at[rows_b, :], local.at[4 + b])

    def normed_block(b):
        for h in range(2):
            rows_b = pl.ds(b * 256 + h * 128, 128)
            for n in range(8):
                cols_n = slice(128 * n, 128 * (n + 1))
                normed[rows_b, cols_n] = (
                    text[rows_b, cols_n].astype(F32) * scol[rows_b, :] * gain_row[:, cols_n]
                ).astype(BF16)
        normed_copy(b).start()

    def order_block(t):
        for k in range(4):
            rows_k = pl.ds(pl.multiple_of(t * SLOTS + k * N_CTX, 32), N_CTX)
            every = pl.ds(t * 4 + k, N_CTX, stride=SLOTS)
            cols[rows_k, 0:128] = colf[every, :].astype(BF16)
            cols[rows_k, 128:160] = colg[every, :][:, 0:32].astype(BF16)

    def add_pair(i, j, first=False):
        base = gg.pair_rows(i, j)
        rows_p = pl.ds(pl.multiple_of(base, 256), 256)
        part = lax.dot_general(
            cols[rows_p, :], gf[rows_p, :], (((0,), (0,)), ((), ())), preferred_element_type=F32
        )
        grad_out[...] = part if first else grad_out[...] + part

    normed_block(0)
    normed_block(1)
    gg.first()
    normed_block(2)
    normed_block(3)
    gg.second()

    @pl.loop(0, N_CTX)
    def _(t):
        order_block(t)

    gg.third(0)
    gg.from_sibling(0, 0)
    add_pair(0, 0, True)
    gg.third(1)
    for i, j in ((1, 0), (0, 1)):
        gg.from_sibling(i, j)
        add_pair(i, j)
    gg.third(2)
    for i, j in ((2, 0), (0, 2)):
        gg.from_sibling(i, j)
        add_pair(i, j)
    gg.third(3)
    for i, j in ((1, 1), (1, 2), (2, 1), (2, 2)):
        gg.from_sibling(i, j)
        add_pair(i, j)
    gg.fourth(0)
    gg.fourth(1)
    for i, j in ((3, 0), (0, 3), (3, 1), (1, 3)):
        gg.from_sibling(i, j)
        add_pair(i, j)
    gg.fourth(2)
    for i, j in ((3, 2), (2, 3)):
        gg.from_sibling(i, j)
        add_pair(i, j)
    gg.fourth(3)
    gg.from_sibling(3, 3)
    add_pair(3, 3)

    for b in range(4):
        normed_copy(b).wait()
    for c in (wg, gg, og, ag):
        c.finish()
    for c in osib:
        c.wait_send()


def shards(
    patches,
    window_ids,
    positions,
    text_embed,
    cotangent,
    qkv_weight,
    out_weight,
    merger_weight,
    norm_gain,
):
    vmem = pl.BlockSpec(memory_space=pltpu.VMEM)
    anywhere = pl.BlockSpec(memory_space=pl.ANY)
    dma = pltpu.SemaphoreType.DMA
    return pl.pallas_call(
        kernel,
        out_shape=(
            jax.ShapeDtypeStruct((TOK, 1024), BF16),
            jax.ShapeDtypeStruct((ROWS_W, 1024), F32),
        ),
        in_specs=[vmem, vmem, vmem, anywhere, anywhere, vmem, anywhere, anywhere, vmem],
        out_specs=(anywhere, vmem),
        scratch_shapes=[
            pltpu.VMEM((N_CTX * ROWS_W, 1024), BF16),
            pltpu.VMEM((N_CTX * SLOTS, 1024), BF16),
            pltpu.VMEM((DV, DV), BF16),
            pltpu.VMEM((DV, 512), BF16),
            pltpu.VMEM((512, DV), BF16),
            pltpu.VMEM((512, DV), BF16),
            pltpu.VMEM((SLOTS, 4 * DV), BF16),
            pltpu.VMEM((4 * DV, SLOTS), BF16),
            pltpu.VMEM((N_CTX, ROWS_W, SLOTS), BF16),
            pltpu.VMEM((N_CTX * SLOTS, 128), F32),
            pltpu.VMEM((N_CTX * SLOTS, 128), F32),
            pltpu.VMEM((N_CTX * SLOTS, ROWS_W), BF16),
            pltpu.VMEM((TOK, 1024), BF16),
            pltpu.VMEM((TOK, 1024), BF16),
            pltpu.VMEM((TOK, 1024), BF16),
            pltpu.VMEM((512, HCOLS), BF16),
            pltpu.VMEM((512, HCOLS), BF16),
            pltpu.VMEM((512, HCOLS), BF16),
            pltpu.VMEM((HCOLS, 512), BF16),
            pltpu.VMEM((512, 128), jnp.int32),
            pltpu.VMEM((SLOTS, 1024), F32),
            pltpu.VMEM((N_CTX, 4, 1024), BF16),
            pltpu.VMEM((N_CTX, 4, 1024), BF16),
            pltpu.VMEM((SLOTS, 1024), F32),
            pltpu.VMEM((N_CTX, 8, SLOTS), jnp.int32),
            pltpu.VMEM((N_CTX, 8, SLOTS), jnp.int32),
            pltpu.VMEM((NZ, 16, SLOTS), F32),
            pltpu.VMEM((SLOTS, 1024), F32),
            pltpu.VMEM((TOK, SLOTS), F32),
            pltpu.VMEM((SLOTS, TOK), BF16),
            dma((8,)),
            dma((36,)), dma((36,)), dma((36,)), dma((36,)),
            dma((8,)), dma((8,)), dma((8,)), dma((8,)), dma((8,)), dma((8,)),
            dma((N_CTX,)), dma((N_CTX,)), dma((N_CTX,)), dma((N_CTX,)), dma((N_CTX,)), dma((N_CTX,)),
            dma((NZ,)), dma((NZ,)),
        ],
        compiler_params=pltpu.CompilerParams(
            collective_id=0, has_side_effects=True, vmem_limit_bytes=62 * 1024 * 1024
        ),
    )(
        patches,
        window_ids.reshape(1, -1),
        positions.reshape(1, -1),
        text_embed,
        cotangent,
        qkv_weight,
        out_weight,
        merger_weight,
        norm_gain.reshape(1, -1),
    )


def solution(mesh):
    in_specs = (
        P("ctx", None),
        P("ctx"),
        P("ctx"),
        P("ctx", "tp"),
        P("ctx", "tp"),
        P(None, None, "tp"),
        P("tp", None),
        P("ctx", "tp"),
        P("tp"),
    )
    out_specs = (P("ctx", "tp"), P("ctx", "tp"))
    return jax.shard_map(shards, mesh=mesh, in_specs=in_specs, out_specs=out_specs, check_vma=False)
```

```python
import jax
import jax.numpy as jnp
from jax import lax
from jax.experimental import pallas as pl
from jax.experimental.pallas import tpu as pltpu
from jax.sharding import PartitionSpec as P

MESH = pl.DeviceIdType.MESH
D = 8192
HEAD_DIM = 80
NX, NY, NC, NZ = 4, 4, 2, 8
N_CTX = 32
SLOTS = 128
TOK = 1024
DV = 1280
HCOLS = 160
ROWS_W = 160
F32 = jnp.float32
BF16 = jnp.bfloat16


def remote(src, dst, send, recv, dev):
    return pltpu.make_async_remote_copy(
        src_ref=src, dst_ref=dst, send_sem=send, recv_sem=recv, device_id=dev, device_id_type=MESH
    )


def dot(a, b):
    return jnp.dot(a, b, preferred_element_type=F32)


def dot_nt(a, b):
    return lax.dot_general(a, b, (((1,), (1,)), ((), ())), preferred_element_type=F32)


def iota(shape, dim):
    return lax.broadcasted_iota(jnp.int32, shape, dim)


class Place:
    def __init__(self):
        self.ctx = lax.axis_index("ctx")
        self.z = lax.axis_index("tp")
        self.core = self.ctx % 2
        y = (self.ctx // 2) % NY
        x = self.ctx // (2 * NY)
        self.f = x * (1 - self.core) + y * self.core
        self.g = y * (1 - self.core) + x * self.core
        self.sib = self.ctx + 1 - 2 * self.core
        self.offs = (0, 3, 1, 2)

    def ctx_of(self, f, g):
        x = f * (1 - self.core) + g * self.core
        y = g * (1 - self.core) + f * self.core
        return (x * NY + y) * 2 + self.core

    def near(self, df, dg):
        return self.ctx_of((self.f + df) % 4, (self.g + dg) % 4)

    def dev(self, df, dg):
        return {"ctx": self.near(df, dg), "tp": self.z}


class PlaneGather:
    def __init__(self, place, buf, rows, ss, rs):
        self.p, self.buf, self.rows, self.half = place, buf, rows, rows // 2
        self.ss, self.rs = ss, rs
        self.started = []

    def block(self, df, dg, part=None):
        base = self.p.near(df, dg) * self.rows
        if part is None:
            return self.buf.at[pl.ds(pl.multiple_of(base, 32), self.rows), :]
        base = base + part * self.half
        return self.buf.at[pl.ds(pl.multiple_of(base, 16), self.half), :]

    def send(self, n, region, dev):
        c = remote(region, region, self.ss.at[n], self.rs.at[n], dev)
        c.start()
        self.started.append(c)

    def recv(self, n, region):
        remote(region, region, self.ss.at[n], self.rs.at[n], self.p.dev(0, 1)).wait_recv()

    def sibling(self, i, j):
        o = self.p.offs
        self.send(20 + 4 * i + j, self.block(o[i], o[j]), {"ctx": self.p.sib, "tp": self.p.z})

    def item(self, i):
        o = self.p.offs
        if i:
            self.sibling(i, 0)
        self.send(4 + 4 * i, self.block(o[i], 0), self.p.dev(0, 1))
        self.send(5 + 4 * i, self.block(o[i], 0), self.p.dev(0, 3))

    def start(self):
        own = self.block(0, 0)
        self.send(0, own, self.p.dev(1, 0))
        self.send(1, own, self.p.dev(3, 0))
        self.sibling(0, 0)

    def first(self):
        self.recv(0, self.block(3, 0))
        self.send(2, self.block(3, 0, 0), self.p.dev(1, 0))
        self.item(0)
        self.item(1)
        self.recv(1, self.block(1, 0))
        self.send(3, self.block(1, 0, 1), self.p.dev(3, 0))
        self.item(2)

    def second(self):
        self.recv(2, self.block(2, 0, 0))
        self.recv(3, self.block(2, 0, 1))
        self.item(3)

    def third(self, i):
        o = self.p.offs[i]
        self.recv(4 + 4 * i, self.block(o, 3))
        self.send(6 + 4 * i, self.block(o, 3, 0), self.p.dev(0, 1))
        self.sibling(i, 1)
        self.recv(5 + 4 * i, self.block(o, 1))
        self.send(7 + 4 * i, self.block(o, 1, 1), self.p.dev(0, 3))
        self.sibling(i, 2)

    def fourth(self, i):
        o = self.p.offs[i]
        self.recv(6 + 4 * i, self.block(o, 2, 0))
        self.recv(7 + 4 * i, self.block(o, 2, 1))
        self.sibling(i, 3)

    def from_sibling(self, i, j):
        o = self.p.offs
        base = self.p.near(o[i], o[j]) + 1 - 2 * self.p.core
        region = self.buf.at[pl.ds(pl.multiple_of(base * self.rows, 32), self.rows), :]
        self.recv(20 + 4 * j + i, region)

    def pair_rows(self, i, j):
        o = self.p.offs
        return (self.p.near(o[i], o[j]) - self.p.core) * self.rows

    def finish(self):
        for c in self.started:
            c.wait_send()


class Ring:
    def __init__(self, place, region, ss, rs):
        self.p, self.region, self.ss, self.rs = place, region, ss, rs
        self.started = []

    def copy(self, s, way):
        part = way if s == 4 else None
        src = (s - 1, (NZ + 1 - s) % NZ)[way]
        dst = (s, NZ - s)[way]
        return remote(
            self.region(src, part), self.region(dst, part), self.ss.at[4 * way + s - 1], self.rs.at[4 * way + s - 1],
            {"ctx": self.p.ctx, "tp": (self.p.z + (1, NZ - 1)[way]) % NZ},
        )

    def step(self, s):
        for way in range(2):
            c = self.copy(s, way)
            c.start()
            self.started.append(c)

    def recv(self, s):
        for way in range(2):
            self.copy(s, way).wait_recv()

    def finish(self):
        for c in self.started:
            c.wait_send()


def kernel(
    pat_in, wid, pos, text_in, cot_in, qkv_in, ow_in, w_in, gain,
    normed_out, grad_out,
    pat, qkv, wf, gf, owf, attf, att_t, att_u, hacc, hid, perm, colsend, colin, colf, colg, cols, text, cot, normed,
    q0s, q1s, ks, vts, widc, mrow, rows_send, rows_in, incf, idx_send, idx_in, stats, cotsel, scol, drow,
    local, w_ss, w_rs, g_ss, g_rs, ow_ss, ow_rs, osib_ss, osib_rs, at_ss, at_rs,
    ix_ss, ix_rs, rw_ss, rw_rs, co_ss, co_rs, cg_ss, cg_rs, st_ss, st_rs,
):
    p = Place()
    ctx, z, core = p.ctx, p.z, p.core

    def other(d):
        return (ctx + d) % N_CTX

    def behind(d):
        return (ctx + N_CTX - d) % N_CTX

    scope = []

    def mark(name):
        if scope:
            scope.pop().__exit__(None, None, None)
        if name:
            scope.append(jax.named_scope(name))
            scope[-1].__enter__()

    mark("index")
    load_pat = pltpu.make_async_copy(pat_in, pat, local.at[8])
    load_qkv = pltpu.make_async_copy(qkv_in, qkv, local.at[9])
    load_pat.start()
    load_qkv.start()

    def block160(ref, c):
        return ref.at[pl.ds(pl.multiple_of(c * ROWS_W, 32), ROWS_W), :]

    barrier = pltpu.get_barrier_semaphore()

    @pl.loop(1, N_CTX)
    def _(d):
        pl.semaphore_signal(barrier, inc=1, device_id={"ctx": other(d), "tp": z}, device_id_type=MESH)

    @pl.loop(1, NZ)
    def _(d):
        pl.semaphore_signal(barrier, inc=1, device_id={"ctx": ctx, "tp": (z + d) % NZ}, device_id_type=MESH)

    own_w = wf.at[pl.ds(pl.multiple_of(ctx * ROWS_W, 32), ROWS_W), :]
    own_ow = owf.at[pl.ds(0, HCOLS), :]
    load_w = pltpu.make_async_copy(w_in, own_w, local.at[0])
    load_ow = pltpu.make_async_copy(ow_in, own_ow, local.at[1])
    load_text = pltpu.make_async_copy(text_in, text, local.at[2])
    load_cot = pltpu.make_async_copy(cot_in, cot, local.at[3])
    load_w.start()
    load_ow.start()
    load_text.start()
    load_cot.start()

    pos_row = pos[...]
    pos_col = jnp.broadcast_to(pos_row, (SLOTS, SLOTS)).T
    t_row = pos_row // TOK
    t_col = pos_col // TOK
    same = t_col == t_row
    earlier_down = same & (iota((SLOTS, SLOTS), 0) < iota((SLOTS, SLOTS), 1))
    earlier_across = same & (iota((SLOTS, SLOTS), 1) < iota((SLOTS, SLOTS), 0))
    rank_row = jnp.sum(jnp.where(earlier_down, 1.0, 0.0).astype(F32), axis=0, keepdims=True)
    rank_col = jnp.sum(jnp.where(earlier_across, 1.0, 0.0).astype(F32), axis=1, keepdims=True)
    live_row = t_row < N_CTX
    bucket_row = jnp.where(live_row, t_row.astype(F32) * 4.0 + rank_row, -1.0)
    to_owner = jnp.where(iota((N_CTX, SLOTS), 0) == t_row, 1.0, 0.0).astype(BF16)
    row_no = pos_col % TOK + 1
    lane_of = rank_col.astype(jnp.int32) * N_CTX + ctx
    at_lane = lane_of == iota((SLOTS, SLOTS), 1)
    high = jnp.where(at_lane, (row_no // 32).astype(F32), 0.0).astype(BF16)
    low = jnp.where(at_lane, (row_no % 32).astype(F32), 0.0).astype(BF16)
    index_rows = (dot(to_owner, high) * 32.0 + dot(to_owner, low)).astype(jnp.int32)
    for t in range(N_CTX):
        idx_send[t] = jnp.broadcast_to(index_rows[t : t + 1, :], (8, SLOTS))
    idx_in[ctx] = idx_send[ctx]

    for b in range(4):
        widc[128 * b : 128 * (b + 1), :] = jnp.broadcast_to(wid[:, 128 * b : 128 * (b + 1)], (128, 128)).T

    mark("qkv")
    load_pat.wait()
    load_qkv.wait()
    patches = pat[...]
    lane = iota((512, HCOLS), 1)
    q = dot_nt(patches, qkv[0]).astype(BF16).astype(F32)
    q0s[...] = jnp.where(lane < HEAD_DIM, q, 0.0).astype(BF16)
    q1s[...] = jnp.where(lane < HEAD_DIM, 0.0, q).astype(BF16)
    ks[...] = dot_nt(patches, qkv[1]).astype(BF16)
    vts[...] = dot_nt(qkv[2], patches).astype(BF16)
    mark("attend")
    factor = 1.0 / HEAD_DIM**0.5

    @pl.loop(0, 4)
    def _(b):
        cols_b = pl.ds(pl.multiple_of(b * 128, 128), 128)
        ids = wid[:, cols_b]
        allowed = (widc[...] == ids) & (widc[...] >= 0)
        parts = []
        for qs in (q0s, q1s):
            scores = dot_nt(ks[...], qs[cols_b, :]) * factor
            scores = jnp.where(allowed, scores, -1e30)
            weights = jnp.exp(scores - jnp.max(scores, axis=0, keepdims=True))
            probs = (weights / jnp.sum(weights, axis=0, keepdims=True)).astype(BF16)
            parts.append(dot(vts[...], probs))
        row = iota((HCOLS, 128), 0)
        attf[0:HCOLS, cols_b] = jnp.where(
            row < HEAD_DIM, parts[0], parts[1]
        ).astype(BF16)

    mark("barrier")
    pl.semaphore_wait(barrier, N_CTX - 1 + NZ - 1)

    wg = PlaneGather(p, wf, ROWS_W, w_ss, w_rs)
    load_w.wait()
    wg.start()

    def place_of(r):
        return r if r < 4 else 7 if r == 4 else r - 1

    def ow_region(r, part):
        base = pl.multiple_of(place_of(r) * HCOLS + core * 80, 16)
        if part is None:
            return owf.at[pl.ds(base, 80), :]
        return owf.at[pl.ds(base, 80), pl.ds(part * 640, 640)]

    def att_region(r, part):
        if part is None:
            return attf.at[pl.ds(place_of(r) * HCOLS, HCOLS), :]
        return attf.at[pl.ds(place_of(r) * HCOLS + part * 80, 80), :]

    osib = []

    def ow_to_sibling(r):
        src = ow_region(r, None)
        c = remote(src, src, osib_ss.at[r], osib_rs.at[r], {"ctx": p.sib, "tp": z})
        c.start()
        osib.append(c)

    def ow_from_sibling(r):
        dst = owf.at[pl.ds(pl.multiple_of(place_of(r) * HCOLS + (1 - core) * 80, 16), 80), :]
        remote(dst, dst, osib_ss.at[r], osib_rs.at[r], {"ctx": p.sib, "tp": z}).wait_recv()

    og = Ring(p, ow_region, ow_ss, ow_rs)
    ag = Ring(p, att_region, at_ss, at_rs)
    load_ow.wait()
    og.step(1)
    ag.step(1)

    mark("w_first")
    wg.first()
    mark("ow1")
    og.recv(1)
    og.step(2)
    mark("at1")
    ag.recv(1)
    ag.step(2)

    @pl.loop(1, N_CTX)
    def _(d):
        remote(
            idx_send.at[other(d)], idx_in.at[ctx], ix_ss.at[d], ix_rs.at[d], {"ctx": other(d), "tp": z}
        ).start()

    mark("w_second")
    wg.second()
    mark("w30")
    wg.third(0)
    mark("ow2")
    og.recv(2)
    og.step(3)
    mark("w31")
    wg.third(1)
    mark("at2")
    ag.recv(2)
    ag.step(3)
    mark("w32")
    wg.third(2)
    mark("ow3")
    og.recv(3)
    og.step(4)
    for r in (1, 7, 2, 6, 3, 5):
        ow_to_sibling(r)
    mark("w33")
    wg.third(3)
    mark("w40")
    wg.fourth(0)
    mark("at3")
    ag.recv(3)
    ag.step(4)
    mark("w41")
    wg.fourth(1)
    mark("ow4")
    og.recv(4)
    ow_to_sibling(4)
    mark("transpose")
    for r in range(7):
        att_t[:, r * HCOLS : (r + 1) * HCOLS] = attf[r * HCOLS : (r + 1) * HCOLS, :].T
    mark("ow_sib")
    for r in (1, 7, 2, 6, 3, 5):
        ow_from_sibling(r)
    mark("out_proj")

    @pl.loop(0, 5)
    def _(n):
        cols_n = pl.ds(pl.multiple_of(n * 256, 256), 256)
        hacc[:, cols_n] = pat[:, cols_n].astype(F32) + dot(att_t[...], owf[0 : 7 * HCOLS, cols_n])

    mark("w42")
    wg.fourth(2)
    wg.fourth(3)
    mark("at4")
    ag.recv(4)
    ow_from_sibling(4)
    mark("hidden")
    att_u[...] = attf[7 * HCOLS : 8 * HCOLS, :].T

    @pl.loop(0, 5)
    def _(n):
        cols_n = pl.ds(pl.multiple_of(n * 256, 256), 256)
        hid[:, cols_n] = (hacc[:, cols_n] + dot(att_u[...], owf[7 * HCOLS : 8 * HCOLS, cols_n])).astype(BF16)

    mark("perm")
    spread_at = jnp.where(iota((SLOTS, 512), 0) == iota((SLOTS, 512), 1) // 4, 1.0, 0.0).astype(BF16)
    bucket512 = dot(jnp.broadcast_to(bucket_row, (8, SLOTS)).astype(BF16), spread_at)[0:1, :]
    chosen = iota((SLOTS, 512), 0).astype(F32) == bucket512
    for i in range(4):
        select = jnp.where(chosen & (iota((SLOTS, 512), 1) % 4 == i), 1.0, 0.0).astype(BF16)
        for n in range(5):
            perm[:, i * DV + n * 256 : i * DV + (n + 1) * 256] = dot(
                select, hid[:, n * 256 : (n + 1) * 256]
            ).astype(BF16)

    mark("w_sib")
    for i in range(4):
        for j in range(4):
            wg.from_sibling(i, j)

    mark("merge")
    @pl.loop(0, 4)
    def _(n):
        cols_n = pl.ds(pl.multiple_of(n * 256, 256), 256)
        mrow[:, cols_n] = dot(perm[...], wf[:, cols_n]).astype(BF16).astype(F32)

    mark("rows_send")
    @pl.loop(0, N_CTX // 2)
    def _(t):
        eight = mrow[pl.ds(pl.multiple_of(t * 8, 8), 8), :]
        rows_send[2 * t] = eight[0:4, :].astype(BF16)
        rows_send[2 * t + 1] = eight[4:8, :].astype(BF16)

    @pl.loop(1, N_CTX)
    def _(d):
        remote(
            rows_send.at[other(d)], rows_in.at[ctx], rw_ss.at[d], rw_rs.at[d], {"ctx": other(d), "tp": z}
        ).start()

    rows_in[ctx] = rows_send[ctx]

    mark("colsend")

    def source(zz, x):
        return (x * NY + (x + zz) % NY) * 2 + zz // NY

    x_here = ctx // (2 * NY)
    turn = ctx == source(z, x_here)

    @pl.when(turn)
    def _():
        for n in range(40):
            colsend[n * 128 : (n + 1) * 128, :] = perm[:, n * 128 : (n + 1) * 128].T

        @pl.loop(1, N_CTX)
        def _(d):
            remote(
                block160(colsend, other(d)), block160(colin, x_here), co_ss.at[d], co_rs.at[x_here],
                {"ctx": other(d), "tp": z},
            ).start()

        colin[pl.ds(pl.multiple_of(x_here * ROWS_W, 32), ROWS_W), :] = colsend[
            pl.ds(pl.multiple_of(ctx * ROWS_W, 32), ROWS_W), :
        ]

    mark("idx_wait")
    @pl.loop(1, N_CTX)
    def _(d):
        remote(
            idx_send.at[other(d)], idx_in.at[behind(d)], ix_ss.at[d], ix_rs.at[d], {"ctx": other(d), "tp": z}
        ).wait()

    mark("cotsel")
    load_text.wait()
    load_cot.wait()
    at_row = (jnp.sum(idx_in[...], axis=0) - 1)[0:1, :]
    at_col = jnp.broadcast_to(at_row, (SLOTS, SLOTS)).T
    for b in range(8):
        drow[:, 128 * b : 128 * (b + 1)] = jnp.where(
            at_col == iota((SLOTS, SLOTS), 1) + 128 * b, 1.0, 0.0
        ).astype(BF16)

    @pl.loop(0, 4)
    def _(n):
        cols_n = pl.ds(pl.multiple_of(n * 256, 256), 256)
        cotsel[:, cols_n] = dot(drow[...], cot[:, cols_n])

    gains = gain[...].astype(F32)

    def gain_of(n):
        return gains[n : n + 1, :]

    def row_sums(rows, cots):
        sq = jnp.zeros((128, 128), F32)
        inner = jnp.zeros((128, 128), F32)
        for n in range(8):
            cols_n = slice(128 * n, 128 * (n + 1))
            x = rows(cols_n)
            sq = sq + x * x
            inner = inner + x * (gain_of(n) * cots(cols_n))
        return jnp.sum(sq.T, axis=0, keepdims=True), jnp.sum(inner.T, axis=0, keepdims=True)

    mark("text_sums")

    @pl.loop(0, 8)
    def _(b):
        rows_b = pl.ds(pl.multiple_of(b * 128, 128), 128)
        sq, inner = row_sums(
            lambda c: text[rows_b, c].astype(F32), lambda c: cot[rows_b, c].astype(F32)
        )
        stats[z, pl.ds(b, 1), :] = sq
        stats[z, pl.ds(8 + b, 1), :] = inner

    mark("rows_wait")

    @pl.loop(1, N_CTX)
    def _(d):
        remote(
            rows_send.at[other(d)], rows_in.at[behind(d)], rw_ss.at[d], rw_rs.at[d], {"ctx": other(d), "tp": z}
        ).wait()

    mark("embed")

    @pl.loop(0, N_CTX, unroll=4)
    def _(s):
        four = rows_in[s].astype(F32)
        for k in range(4):
            incf[pl.ds(k * N_CTX + s, 1), :] = four[k : k + 1, :]

    mark("new_sums")
    sq_new, inner_new = row_sums(lambda c: incf[:, c], lambda c: cotsel[:, c])
    sq_new = jnp.broadcast_to(sq_new, (SLOTS, SLOTS)).T
    inner_new = jnp.broadcast_to(inner_new, (SLOTS, SLOTS)).T
    for b in range(8):
        here = at_col == iota((SLOTS, SLOTS), 1) + 128 * b
        taken = jnp.sum(jnp.where(here, 1.0, 0.0), axis=0, keepdims=True) > 0.0
        for base, new in ((b, sq_new), (8 + b, inner_new)):
            put = jnp.sum(jnp.where(here, new, 0.0), axis=0, keepdims=True)
            stats[z, base : base + 1, :] = jnp.where(taken, put, stats[z, base : base + 1, :])

    def stat_copy(d, slot):
        return remote(
            stats.at[z], stats.at[slot], st_ss.at[d], st_rs.at[d], {"ctx": ctx, "tp": (z + d) % NZ}
        )

    mark("stat")

    @pl.loop(1, NZ)
    def _(d):
        stat_copy(d, z).start()

    mark("place")
    inc = incf[...].astype(BF16)

    @pl.loop(0, 8)
    def _(b):
        rows_b = pl.ds(pl.multiple_of(b * 128, 128), 128)
        placed = jnp.where(iota((128, SLOTS), 0) + 128 * b == at_row, 1.0, 0.0).astype(F32)
        taken = jnp.sum(placed, axis=1, keepdims=True) > 0.0
        vision = dot(placed.astype(BF16), inc)
        for n in range(8):
            cols_n = slice(128 * n, 128 * (n + 1))
            text[rows_b, cols_n] = jnp.where(taken, vision[:, cols_n].astype(BF16), text[rows_b, cols_n])

    mark("stat_wait")

    @pl.loop(1, NZ)
    def _(d):
        stat_copy(d, (z + NZ - d) % NZ).wait()

    mark("drows")
    total = jnp.sum(stats[...], axis=0)
    scale = lax.rsqrt(total[0:8, :] / D + 1e-06)
    inner_all = total[8:16, :]
    scale_at = jnp.zeros((1, SLOTS), F32)
    inner_at = jnp.zeros((1, SLOTS), F32)
    for b in range(8):
        here = iota((128, SLOTS), 0) + 128 * b == at_row
        scale_b = jnp.broadcast_to(scale[b : b + 1, :], (128, 128)).T
        inner_b = jnp.broadcast_to(inner_all[b : b + 1, :], (128, 128)).T
        scol[128 * b : 128 * (b + 1), :] = scale_b
        scale_at = scale_at + jnp.sum(jnp.where(here, scale_b, 0.0), axis=0, keepdims=True)
        inner_at = inner_at + jnp.sum(jnp.where(here, inner_b, 0.0), axis=0, keepdims=True)
    s_at = jnp.broadcast_to(scale_at, (SLOTS, SLOTS)).T
    i_at = jnp.broadcast_to(inner_at, (SLOTS, SLOTS)).T
    own_g = pl.ds(pl.multiple_of(ctx * SLOTS, 128), SLOTS)
    for n in range(8):
        cols_n = slice(128 * n, 128 * (n + 1))
        gained = gain_of(n) * cotsel[:, cols_n]
        gf[own_g, cols_n] = (s_at * gained - incf[:, cols_n] * (s_at * s_at * s_at) * i_at / D).astype(BF16)

    gg = PlaneGather(p, gf, SLOTS, g_ss, g_rs)
    gg.start()

    def normed_copy(b):
        rows_b = pl.ds(pl.multiple_of(b * 256, 256), 256)
        return pltpu.make_async_copy(normed.at[rows_b, :], normed_out.at[rows_b, :], local.at[4 + b])

    def normed_block(b):
        for h in range(2):
            rows_b = pl.ds(b * 256 + h * 128, 128)
            for n in range(8):
                cols_n = slice(128 * n, 128 * (n + 1))
                normed[rows_b, cols_n] = (
                    text[rows_b, cols_n].astype(F32) * scol[rows_b, :] * gain_of(n)
                ).astype(BF16)
        normed_copy(b).start()

    def order_block(t):
        for k in range(4):
            rows_k = pl.ds(pl.multiple_of(t * SLOTS + k * N_CTX, 32), N_CTX)
            every = pl.ds(t * 4 + k, N_CTX, stride=SLOTS)
            cols[rows_k, 0:128] = colf[every, :].astype(BF16)
            cols[rows_k, 128:160] = colg[every, :][:, 0:32].astype(BF16)

    def add_pair(i, j, first=False):
        base = gg.pair_rows(i, j)
        rows_p = pl.ds(pl.multiple_of(base, 256), 256)
        part = lax.dot_general(
            cols[rows_p, :], gf[rows_p, :], (((0,), (0,)), ((), ())), preferred_element_type=F32
        )
        grad_out[...] = part if first else grad_out[...] + part

    def col_region(r, part):
        if part is None:
            return colin.at[pl.ds(r * 640, 640), :]
        return colin.at[pl.ds(r * 640 + part * 320, 320), :]

    cg = Ring(p, col_region, cg_ss, cg_rs)

    def turn_cols(r):
        @pl.loop(0, 4)
        def _(x):
            rows_s = pl.ds(pl.multiple_of(source((z + NZ - r) % NZ, x) * SLOTS, 128), SLOTS)
            came = colin[pl.ds(pl.multiple_of((r * 4 + x) * ROWS_W, 32), ROWS_W), :].astype(F32)
            colf[rows_s, :] = came[0:128, :].T
            colg[rows_s, :] = jnp.concatenate([came[128:160, :], jnp.zeros((96, 128), F32)], axis=0).T

    mark("col_wait")
    for j in range(4):

        @pl.when(ctx != source(z, j))
        def _():
            remote(
                block160(colsend, ctx), block160(colin, j), co_ss.at[0], co_rs.at[j], {"ctx": p.sib, "tp": z}
            ).wait_recv()

    cg.step(1)
    mark("normed")
    normed_block(0)
    normed_block(1)
    normed_block(2)
    normed_block(3)
    turn_cols(0)
    mark("g1")
    gg.first()
    mark("c1")
    cg.recv(1)
    cg.step(2)
    mark("col_t")
    turn_cols(1)
    turn_cols(7)
    mark("g2")
    gg.second()
    mark("c2")
    cg.recv(2)
    cg.step(3)
    mark("g30")
    gg.third(0)
    mark("col_t")
    turn_cols(2)
    turn_cols(6)
    mark("g31")
    gg.third(1)
    mark("c3")
    cg.recv(3)
    cg.step(4)
    mark("col_t")
    turn_cols(3)
    turn_cols(5)
    mark("g32")
    gg.third(2)
    mark("c4")
    cg.recv(4)
    mark("col_t")
    turn_cols(4)
    mark("order")

    @pl.loop(0, N_CTX)
    def _(t):
        order_block(t)

    mark("add1")
    gg.from_sibling(0, 0)
    add_pair(0, 0, True)
    for i, j in ((1, 0), (0, 1)):
        gg.from_sibling(i, j)
        add_pair(i, j)
    for i, j in ((2, 0), (0, 2)):
        gg.from_sibling(i, j)
        add_pair(i, j)
    mark("g33")
    gg.third(3)
    for i, j in ((1, 1), (1, 2), (2, 1), (2, 2)):
        gg.from_sibling(i, j)
        add_pair(i, j)
    mark("g40")
    gg.fourth(0)
    gg.fourth(1)
    for i, j in ((3, 0), (0, 3), (3, 1), (1, 3)):
        gg.from_sibling(i, j)
        add_pair(i, j)
    mark("g42")
    gg.fourth(2)
    for i, j in ((3, 2), (2, 3)):
        gg.from_sibling(i, j)
        add_pair(i, j)
    mark("g43")
    gg.fourth(3)
    gg.from_sibling(3, 3)
    add_pair(3, 3)

    mark("end")
    for b in range(4):
        normed_copy(b).wait()
    for c in (wg, gg, og, ag, cg):
        c.finish()
    for c in osib:
        c.wait_send()

    @pl.when(turn)
    def _():
        @pl.loop(1, N_CTX)
        def _(d):
            remote(
                block160(colsend, other(d)), block160(colin, x_here), co_ss.at[d], co_rs.at[0], {"ctx": other(d), "tp": z}
            ).wait_send()

    mark(None)


def hand_out(normed_in, grad_in, normed_out, grad_out, normed, grad, sem_in, sem_out):
    parts = [
        (normed_in.at[pl.ds(r, 256), :], normed.at[pl.ds(r, 256), :], normed_out.at[pl.ds(r, 256), :])
        for r in range(0, TOK, 256)
    ] + [(grad_in, grad, grad_out)]
    come = [pltpu.make_async_copy(a, b, sem_in.at[n]) for n, (a, b, _) in enumerate(parts)]
    go = [pltpu.make_async_copy(b, c, sem_out.at[n]) for n, (_, b, c) in enumerate(parts)]
    for c in come:
        c.start()
    for c, g in zip(come, go):
        c.wait()
        g.start()
    for g in go:
        g.wait()


def shards(
    patches,
    window_ids,
    positions,
    text_embed,
    cotangent,
    qkv_weight,
    out_weight,
    merger_weight,
    norm_gain,
):
    vmem = pl.BlockSpec(memory_space=pltpu.VMEM)
    anywhere = pl.BlockSpec(memory_space=pl.ANY)
    dma = pltpu.SemaphoreType.DMA
    outs = pl.pallas_call(
        kernel,
        out_shape=(
            jax.ShapeDtypeStruct((TOK, 1024), BF16),
            jax.ShapeDtypeStruct((ROWS_W, 1024), F32),
        ),
        in_specs=[anywhere, vmem, vmem, anywhere, anywhere, anywhere, anywhere, anywhere, vmem],
        out_specs=(anywhere, vmem),
        scratch_shapes=[
            pltpu.VMEM((512, DV), BF16),
            pltpu.VMEM((3, HCOLS, DV), BF16),
            pltpu.VMEM((N_CTX * ROWS_W, 1024), BF16),
            pltpu.VMEM((N_CTX * SLOTS, 1024), BF16),
            pltpu.VMEM((DV, DV), BF16),
            pltpu.VMEM((DV, 512), BF16),
            pltpu.VMEM((512, 7 * HCOLS), BF16),
            pltpu.VMEM((512, HCOLS), BF16),
            pltpu.VMEM((512, DV), F32),
            pltpu.VMEM((512, DV), BF16),
            pltpu.VMEM((SLOTS, 4 * DV), BF16),
            pltpu.VMEM((4 * DV, SLOTS), BF16),
            pltpu.VMEM((N_CTX * ROWS_W, SLOTS), BF16),
            pltpu.VMEM((N_CTX * SLOTS, 128), F32),
            pltpu.VMEM((N_CTX * SLOTS, 128), F32),
            pltpu.VMEM((N_CTX * SLOTS, ROWS_W), BF16),
            pltpu.VMEM((TOK, 1024), BF16),
            pltpu.VMEM((TOK, 1024), BF16),
            pltpu.VMEM((TOK, 1024), BF16),
            pltpu.VMEM((512, HCOLS), BF16),
            pltpu.VMEM((512, HCOLS), BF16),
            pltpu.VMEM((512, HCOLS), BF16),
            pltpu.VMEM((HCOLS, 512), BF16),
            pltpu.VMEM((512, 128), jnp.int32),
            pltpu.VMEM((SLOTS, 1024), F32),
            pltpu.VMEM((N_CTX, 4, 1024), BF16),
            pltpu.VMEM((N_CTX, 4, 1024), BF16),
            pltpu.VMEM((SLOTS, 1024), F32),
            pltpu.VMEM((N_CTX, 8, SLOTS), jnp.int32),
            pltpu.VMEM((N_CTX, 8, SLOTS), jnp.int32),
            pltpu.VMEM((NZ, 16, SLOTS), F32),
            pltpu.VMEM((SLOTS, 1024), F32),
            pltpu.VMEM((TOK, SLOTS), F32),
            pltpu.VMEM((SLOTS, TOK), BF16),
            dma((10,)),
            dma((36,)), dma((36,)), dma((36,)), dma((36,)),
            dma((8,)), dma((8,)), dma((8,)), dma((8,)), dma((8,)), dma((8,)),
            dma((N_CTX,)), dma((N_CTX,)), dma((N_CTX,)), dma((N_CTX,)), dma((N_CTX,)), dma((4,)), dma((8,)), dma((8,)),
            dma((NZ,)), dma((NZ,)),
        ],
        compiler_params=pltpu.CompilerParams(
            collective_id=0, has_side_effects=True, vmem_limit_bytes=62 * 1024 * 1024
        ),
    )(
        patches,
        window_ids.reshape(1, -1),
        positions.reshape(1, -1),
        text_embed,
        cotangent,
        jnp.swapaxes(qkv_weight, 1, 2),
        out_weight,
        merger_weight,
        norm_gain.reshape(8, 128),
    )
    return pl.pallas_call(
        hand_out,
        out_shape=(
            jax.ShapeDtypeStruct((TOK, 1024), BF16),
            jax.ShapeDtypeStruct((ROWS_W, 1024), F32),
        ),
        in_specs=[anywhere, anywhere],
        out_specs=(anywhere, anywhere),
        scratch_shapes=[
            pltpu.VMEM((TOK, 1024), BF16),
            pltpu.VMEM((ROWS_W, 1024), F32),
            dma((5,)),
            dma((5,)),
        ],
    )(*outs)


def solution(mesh):
    in_specs = (
        P("ctx", None),
        P("ctx"),
        P("ctx"),
        P("ctx", "tp"),
        P("ctx", "tp"),
        P(None, None, "tp"),
        P("tp", None),
        P("ctx", "tp"),
        P("tp"),
    )
    out_specs = (P("ctx", "tp"), P("ctx", "tp"))
    return jax.shard_map(shards, mesh=mesh, in_specs=in_specs, out_specs=out_specs, check_vma=False)
```

```python
import jax
import jax.numpy as jnp
from jax import lax
from jax.experimental import pallas as pl
from jax.experimental.pallas import tpu as pltpu
from jax.sharding import PartitionSpec as P

MESH = pl.DeviceIdType.MESH
D = 8192
HEAD_DIM = 80
NX, NY, NC, NZ = 4, 4, 2, 8
N_CTX = 32
SLOTS = 128
TOK = 1024
DV = 1280
HCOLS = 160
ROWS_W = 160
PITCH = 136
F32 = jnp.float32
BF16 = jnp.bfloat16


def remote(src, dst, send, recv, dev):
    return pltpu.make_async_remote_copy(
        src_ref=src, dst_ref=dst, send_sem=send, recv_sem=recv, device_id=dev, device_id_type=MESH
    )


def dot(a, b):
    return jnp.dot(a, b, preferred_element_type=F32)


def dot_nt(a, b):
    return lax.dot_general(a, b, (((1,), (1,)), ((), ())), preferred_element_type=F32)


def iota(shape, dim):
    return lax.broadcasted_iota(jnp.int32, shape, dim)


class Place:
    def __init__(self):
        self.ctx = lax.axis_index("ctx")
        self.z = lax.axis_index("tp")
        self.core = self.ctx % 2
        y = (self.ctx // 2) % NY
        x = self.ctx // (2 * NY)
        self.f = x * (1 - self.core) + y * self.core
        self.g = y * (1 - self.core) + x * self.core
        self.sib = self.ctx + 1 - 2 * self.core
        self.offs = (0, 3, 1, 2)

    def ctx_of(self, f, g):
        x = f * (1 - self.core) + g * self.core
        y = g * (1 - self.core) + f * self.core
        return (x * NY + y) * 2 + self.core

    def near(self, df, dg):
        return self.ctx_of((self.f + df) % 4, (self.g + dg) % 4)

    def dev(self, df, dg):
        return {"ctx": self.near(df, dg), "tp": self.z}


class PlaneGather:
    def __init__(self, place, buf, rows, ss, rs):
        self.p, self.buf, self.rows, self.half = place, buf, rows, rows // 2
        self.ss, self.rs = ss, rs
        self.started = []

    def block(self, df, dg, part=None):
        base = self.p.near(df, dg) * self.rows
        if part is None:
            return self.buf.at[pl.ds(pl.multiple_of(base, 32), self.rows), :]
        base = base + part * self.half
        return self.buf.at[pl.ds(pl.multiple_of(base, 16), self.half), :]

    def send(self, n, region, dev):
        c = remote(region, region, self.ss.at[n], self.rs.at[n], dev)
        c.start()
        self.started.append(c)

    def recv(self, n, region):
        remote(region, region, self.ss.at[n], self.rs.at[n], self.p.dev(0, 1)).wait_recv()

    def sibling(self, i, j):
        o = self.p.offs
        self.send(20 + 4 * i + j, self.block(o[i], o[j]), {"ctx": self.p.sib, "tp": self.p.z})

    def item(self, i):
        o = self.p.offs
        if i:
            self.sibling(i, 0)
        self.send(4 + 4 * i, self.block(o[i], 0), self.p.dev(0, 1))
        self.send(5 + 4 * i, self.block(o[i], 0), self.p.dev(0, 3))

    def start(self):
        own = self.block(0, 0)
        self.send(0, own, self.p.dev(1, 0))
        self.send(1, own, self.p.dev(3, 0))
        self.item(0)
        self.sibling(0, 0)

    def first(self):
        self.recv(0, self.block(3, 0))
        self.send(2, self.block(3, 0, 0), self.p.dev(1, 0))
        self.item(1)
        self.recv(1, self.block(1, 0))
        self.send(3, self.block(1, 0, 1), self.p.dev(3, 0))
        self.item(2)

    def second(self):
        self.recv(2, self.block(2, 0, 0))
        self.recv(3, self.block(2, 0, 1))
        self.item(3)

    def third(self, i):
        o = self.p.offs[i]
        self.recv(4 + 4 * i, self.block(o, 3))
        self.send(6 + 4 * i, self.block(o, 3, 0), self.p.dev(0, 1))
        self.sibling(i, 1)
        self.recv(5 + 4 * i, self.block(o, 1))
        self.send(7 + 4 * i, self.block(o, 1, 1), self.p.dev(0, 3))
        self.sibling(i, 2)

    def fourth(self, i):
        o = self.p.offs[i]
        self.recv(6 + 4 * i, self.block(o, 2, 0))
        self.recv(7 + 4 * i, self.block(o, 2, 1))
        self.sibling(i, 3)

    def from_sibling(self, i, j):
        o = self.p.offs
        base = self.p.near(o[i], o[j]) + 1 - 2 * self.p.core
        region = self.buf.at[pl.ds(pl.multiple_of(base * self.rows, 32), self.rows), :]
        self.recv(20 + 4 * j + i, region)

    def pair_rows(self, i, j):
        o = self.p.offs
        return (self.p.near(o[i], o[j]) - self.p.core) * self.rows

    def finish(self):
        for c in self.started:
            c.wait_send()


class Ring:
    def __init__(self, place, region, ss, rs):
        self.p, self.region, self.ss, self.rs = place, region, ss, rs
        self.started = []

    def copy(self, s, way):
        part = way if s == 4 else None
        src = (s - 1, (NZ + 1 - s) % NZ)[way]
        dst = (s, NZ - s)[way]
        return remote(
            self.region(src, part), self.region(dst, part), self.ss.at[4 * way + s - 1], self.rs.at[4 * way + s - 1],
            {"ctx": self.p.ctx, "tp": (self.p.z + (1, NZ - 1)[way]) % NZ},
        )

    def step(self, s):
        for way in range(2):
            c = self.copy(s, way)
            c.start()
            self.started.append(c)

    def recv(self, s):
        for way in range(2):
            self.copy(s, way).wait_recv()

    def finish(self):
        for c in self.started:
            c.wait_send()


def kernel(
    pat_in, wid, pos, text_in, cot_in, qkv_in, ow_in, w_in, gain,
    normed_out, grad_out,
    pat, qkv, wf, gf, owf, attf, att_t, att_u, hacc, hid, perm, colsend, colin, colf, colg, cols, text, cot, normed,
    q0s, q1s, ks, vts, widc, mrow, rows_send, rows_in, incf, idx_send, idx_in, stats, cotsel, scol, drow,
    local, w_ss, w_rs, g_ss, g_rs, ow_ss, ow_rs, osib_ss, osib_rs, at_ss, at_rs,
    ix_ss, ix_rs, rw_ss, rw_rs, co_ss, co_rs, cg_ss, cg_rs, st_ss, st_rs,
):
    p = Place()
    ctx, z, core = p.ctx, p.z, p.core

    def other(d):
        return (ctx + d) % N_CTX

    def behind(d):
        return (ctx + N_CTX - d) % N_CTX

    scope = []

    def mark(name):
        if scope:
            scope.pop().__exit__(None, None, None)
        if name:
            scope.append(jax.named_scope(name))
            scope[-1].__enter__()

    mark("index")
    load_pat = pltpu.make_async_copy(pat_in, pat, local.at[8])
    load_qkv = pltpu.make_async_copy(qkv_in, qkv, local.at[9])
    load_pat.start()
    load_qkv.start()

    def block160(ref, c):
        return ref.at[pl.ds(pl.multiple_of(c * ROWS_W, 32), ROWS_W), :]

    barrier = pltpu.get_barrier_semaphore()

    @pl.loop(1, N_CTX)
    def _(d):
        pl.semaphore_signal(barrier, inc=1, device_id={"ctx": other(d), "tp": z}, device_id_type=MESH)

    @pl.loop(1, NZ)
    def _(d):
        pl.semaphore_signal(barrier, inc=1, device_id={"ctx": ctx, "tp": (z + d) % NZ}, device_id_type=MESH)

    own_w = wf.at[pl.ds(pl.multiple_of(ctx * ROWS_W, 32), ROWS_W), :]
    own_ow = owf.at[pl.ds(0, HCOLS), :]
    load_w = pltpu.make_async_copy(w_in, own_w, local.at[0])
    load_ow = pltpu.make_async_copy(ow_in, own_ow, local.at[1])
    load_text = pltpu.make_async_copy(text_in, text, local.at[2])
    load_cot = pltpu.make_async_copy(cot_in, cot, local.at[3])
    load_w.start()
    load_ow.start()
    load_text.start()
    load_cot.start()

    pos_row = pos[...]
    pos_col = jnp.broadcast_to(pos_row, (SLOTS, SLOTS)).T
    t_row = pos_row // TOK
    t_col = pos_col // TOK
    same = t_col == t_row
    earlier_down = same & (iota((SLOTS, SLOTS), 0) < iota((SLOTS, SLOTS), 1))
    earlier_across = same & (iota((SLOTS, SLOTS), 1) < iota((SLOTS, SLOTS), 0))
    rank_row = jnp.sum(jnp.where(earlier_down, 1.0, 0.0).astype(F32), axis=0, keepdims=True)
    rank_col = jnp.sum(jnp.where(earlier_across, 1.0, 0.0).astype(F32), axis=1, keepdims=True)
    live_row = t_row < N_CTX
    bucket_row = jnp.where(live_row, t_row.astype(F32) * 4.0 + rank_row, -1.0)
    to_owner = jnp.where(iota((N_CTX, SLOTS), 0) == t_row, 1.0, 0.0).astype(BF16)
    row_no = pos_col % TOK + 1
    lane_of = rank_col.astype(jnp.int32) * N_CTX + ctx
    at_lane = lane_of == iota((SLOTS, SLOTS), 1)
    high = jnp.where(at_lane, (row_no // 32).astype(F32), 0.0).astype(BF16)
    low = jnp.where(at_lane, (row_no % 32).astype(F32), 0.0).astype(BF16)
    index_rows = (dot(to_owner, high) * 32.0 + dot(to_owner, low)).astype(jnp.int32)
    for t in range(N_CTX):
        idx_send[t] = jnp.broadcast_to(index_rows[t : t + 1, :], (8, SLOTS))
    idx_in[ctx] = idx_send[ctx]

    for b in range(4):
        widc[128 * b : 128 * (b + 1), :] = jnp.broadcast_to(wid[:, 128 * b : 128 * (b + 1)], (128, 128)).T

    mark("qkv")
    load_pat.wait()
    load_qkv.wait()
    patches = pat[...]
    lane = iota((512, HCOLS), 1)
    q = dot_nt(patches, qkv[0]).astype(BF16).astype(F32)
    q0s[...] = jnp.where(lane < HEAD_DIM, q, 0.0).astype(BF16)
    q1s[...] = jnp.where(lane < HEAD_DIM, 0.0, q).astype(BF16)
    ks[...] = dot_nt(patches, qkv[1]).astype(BF16)
    vts[...] = dot_nt(qkv[2], patches).astype(BF16)
    mark("barrier")
    pl.semaphore_wait(barrier, N_CTX - 1 + NZ - 1)

    wg = PlaneGather(p, wf, ROWS_W, w_ss, w_rs)
    load_w.wait()
    wg.start()

    def place_of(r):
        return (0, 1, 7, 2, 6, 3, 5, 4).index(r)

    def ow_region(r, part):
        base = pl.multiple_of(place_of(r) * HCOLS + core * 80, 16)
        if part is None:
            return owf.at[pl.ds(base, 80), :]
        return owf.at[pl.ds(base, 80), pl.ds(part * 640, 640)]

    def att_region(r, part):
        if part is None:
            return attf.at[pl.ds(place_of(r) * HCOLS, HCOLS), :]
        return attf.at[pl.ds(place_of(r) * HCOLS + part * 80, 80), :]

    osib = []

    def ow_to_sibling(r):
        src = ow_region(r, None)
        c = remote(src, src, osib_ss.at[r], osib_rs.at[r], {"ctx": p.sib, "tp": z})
        c.start()
        osib.append(c)

    def ow_from_sibling(r):
        dst = owf.at[pl.ds(pl.multiple_of(place_of(r) * HCOLS + (1 - core) * 80, 16), 80), :]
        remote(dst, dst, osib_ss.at[r], osib_rs.at[r], {"ctx": p.sib, "tp": z}).wait_recv()

    og = Ring(p, ow_region, ow_ss, ow_rs)
    ag = Ring(p, att_region, at_ss, at_rs)
    load_ow.wait()
    og.step(1)
    mark("attend")
    factor = 1.0 / HEAD_DIM**0.5

    @pl.loop(0, 4)
    def _(b):
        cols_b = pl.ds(pl.multiple_of(b * 128, 128), 128)
        ids = wid[:, cols_b]
        allowed = (widc[...] == ids) & (widc[...] >= 0)
        parts = []
        for qs in (q0s, q1s):
            scores = dot_nt(ks[...], qs[cols_b, :]) * factor
            scores = jnp.where(allowed, scores, -1e30)
            weights = jnp.exp(scores - jnp.max(scores, axis=0, keepdims=True))
            probs = (weights / jnp.sum(weights, axis=0, keepdims=True)).astype(BF16)
            parts.append(dot(vts[...], probs))
        row = iota((HCOLS, 128), 0)
        attf[0:HCOLS, cols_b] = jnp.where(
            row < HEAD_DIM, parts[0], parts[1]
        ).astype(BF16)

    ag.step(1)

    def turn_att(r):
        k = place_of(r)
        part = attf[k * HCOLS : (k + 1) * HCOLS, :].T
        if k < 5:
            att_t[:, k * HCOLS : (k + 1) * HCOLS] = part
        else:
            att_u[:, (k - 5) * HCOLS : (k - 4) * HCOLS] = part

    def near_product(n):
        cols_n = slice(n * 256, (n + 1) * 256)
        hacc[:, cols_n] = pat[:, cols_n].astype(F32) + dot(att_t[...], owf[0 : 5 * HCOLS, cols_n])

    turn_att(0)
    mark("ow1")
    og.recv(1)
    og.step(2)
    ow_to_sibling(1)
    ow_to_sibling(7)
    mark("w_first")
    wg.first()
    mark("w30")
    wg.third(0)
    mark("at1")
    ag.recv(1)
    ag.step(2)
    turn_att(1)
    turn_att(7)

    @pl.loop(1, N_CTX)
    def _(d):
        remote(
            idx_send.at[other(d)], idx_in.at[ctx], ix_ss.at[d], ix_rs.at[d], {"ctx": other(d), "tp": z}
        ).start()

    mark("w_second")
    wg.second()
    mark("ow2")
    og.recv(2)
    og.step(3)
    ow_to_sibling(2)
    ow_to_sibling(6)
    mark("w31")
    wg.third(1)
    mark("at2")
    ag.recv(2)
    ag.step(3)
    turn_att(2)
    turn_att(6)
    for r in (1, 7, 2, 6):
        ow_from_sibling(r)
    near_product(0)
    mark("w32")
    wg.third(2)
    near_product(1)
    mark("ow3")
    og.recv(3)
    og.step(4)
    ow_to_sibling(3)
    ow_to_sibling(5)
    near_product(2)
    mark("w33")
    wg.third(3)
    mark("w40")
    wg.fourth(0)
    mark("at3")
    ag.recv(3)
    ag.step(4)
    near_product(3)
    turn_att(3)
    turn_att(5)
    mark("w41")
    wg.fourth(1)
    near_product(4)
    mark("ow4")
    og.recv(4)
    ow_to_sibling(4)
    mark("w42")
    wg.fourth(2)
    wg.fourth(3)
    for r in (3, 5):
        ow_from_sibling(r)
    mark("at4")
    ag.recv(4)
    ow_from_sibling(4)
    mark("hidden")
    turn_att(4)

    @pl.loop(0, 5)
    def _(n):
        cols_n = pl.ds(pl.multiple_of(n * 256, 256), 256)
        hid[:, cols_n] = (hacc[:, cols_n] + dot(att_u[...], owf[5 * HCOLS : 8 * HCOLS, cols_n])).astype(BF16)

    mark("perm")
    spread_at = jnp.where(iota((SLOTS, 512), 0) == iota((SLOTS, 512), 1) // 4, 1.0, 0.0).astype(BF16)
    bucket512 = dot(jnp.broadcast_to(bucket_row, (8, SLOTS)).astype(BF16), spread_at)[0:1, :]
    chosen = iota((SLOTS, 512), 0).astype(F32) == bucket512
    for i in range(4):
        select = jnp.where(chosen & (iota((SLOTS, 512), 1) % 4 == i), 1.0, 0.0).astype(BF16)
        for n in range(5):
            perm[:, i * DV + n * 256 : i * DV + (n + 1) * 256] = dot(
                select, hid[:, n * 256 : (n + 1) * 256]
            ).astype(BF16)

    mark("w_sib")
    for i in range(4):
        for j in range(4):
            wg.from_sibling(i, j)

    mark("merge")
    @pl.loop(0, 4)
    def _(n):
        cols_n = pl.ds(pl.multiple_of(n * 256, 256), 256)
        mrow[:, cols_n] = dot(perm[...], wf[:, cols_n]).astype(BF16).astype(F32)

    mark("rows_send")
    @pl.loop(0, N_CTX // 2)
    def _(t):
        eight = mrow[pl.ds(pl.multiple_of(t * 8, 8), 8), :]
        rows_send[2 * t] = eight[0:4, :].astype(BF16)
        rows_send[2 * t + 1] = eight[4:8, :].astype(BF16)

    def at_offset(dx, dy, dc):
        x = (ctx // (2 * NY) + dx) % NX
        y = ((ctx // 2) % NY + dy) % NY
        return (x * NY + y) * 2 + (core + dc) % 2

    hops = (0, 1, 2, 1)
    offsets = sorted(
        ((dx, dy, dc) for dx in range(4) for dy in range(4) for dc in range(2) if dx + dy + dc > 0),
        key=lambda o: (-hops[o[0]] - hops[o[1]], o),
    )

    def row_copy(n, arriving):
        dx, dy, dc = offsets[n]
        to = at_offset(dx, dy, dc)
        slot = at_offset(-dx % 4, -dy % 4, dc) if arriving else ctx
        return remote(rows_send.at[to], rows_in.at[slot], rw_ss.at[n], rw_rs.at[n], {"ctx": to, "tp": z})

    for n in range(len(offsets)):
        row_copy(n, False).start()

    rows_in[ctx] = rows_send[ctx]

    mark("colsend")

    def source(zz, x):
        return (x * NY + (x + zz) % NY) * 2 + zz // NY

    x_here = ctx // (2 * NY)
    plane = (z - ((ctx // 2) % NY - x_here + NY) % NY - NY * core + NZ) % NZ
    turn = (plane == 0) | (plane == 2)
    half = plane // 2

    def half_block(c, slot):
        return (
            colsend.at[pl.ds(pl.multiple_of(c * ROWS_W + (half % 2) * 80, 16), 80), :],
            colin.at[pl.ds(pl.multiple_of(slot * 80, 16), 80), :],
        )

    def col_copy(n):
        to = at_offset(*offsets[n])
        slot = (half % 2) * 4 + x_here
        src, dst = half_block(to, slot)
        return remote(src, dst, co_ss.at[n], co_rs.at[slot], {"ctx": to, "tp": z})

    @pl.when(turn)
    def _():
        for n in range(40):
            colsend[n * 128 : (n + 1) * 128, :] = perm[:, n * 128 : (n + 1) * 128].T

        for n in range(len(offsets)):
            col_copy(n).start()
        mine = pl.ds(pl.multiple_of(ctx * ROWS_W + (half % 2) * 80, 16), 80)
        colin[pl.ds(pl.multiple_of(((half % 2) * 4 + x_here) * 80, 16), 80), :] = colsend[mine, :]

    mark("idx_wait")
    @pl.loop(1, N_CTX)
    def _(d):
        remote(
            idx_send.at[other(d)], idx_in.at[behind(d)], ix_ss.at[d], ix_rs.at[d], {"ctx": other(d), "tp": z}
        ).wait()

    mark("cotsel")
    load_text.wait()
    load_cot.wait()
    at_row = (jnp.sum(idx_in[...], axis=0) - 1)[0:1, :]
    at_col = jnp.broadcast_to(at_row, (SLOTS, SLOTS)).T
    for b in range(8):
        drow[:, 128 * b : 128 * (b + 1)] = jnp.where(
            at_col == iota((SLOTS, SLOTS), 1) + 128 * b, 1.0, 0.0
        ).astype(BF16)

    @pl.loop(0, 4)
    def _(n):
        cols_n = pl.ds(pl.multiple_of(n * 256, 256), 256)
        cotsel[:, cols_n] = dot(drow[...], cot[:, cols_n])

    gains = gain[...].astype(F32)

    def gain_of(n):
        return gains[n : n + 1, :]

    def row_sums(rows, cots):
        sq = jnp.zeros((128, 128), F32)
        inner = jnp.zeros((128, 128), F32)
        for n in range(8):
            cols_n = slice(128 * n, 128 * (n + 1))
            x = rows(cols_n)
            sq = sq + x * x
            inner = inner + x * (gain_of(n) * cots(cols_n))
        return jnp.sum(sq.T, axis=0, keepdims=True), jnp.sum(inner.T, axis=0, keepdims=True)

    mark("text_sums")

    @pl.loop(0, 8)
    def _(b):
        rows_b = pl.ds(pl.multiple_of(b * 128, 128), 128)
        sq, inner = row_sums(
            lambda c: text[rows_b, c].astype(F32), lambda c: cot[rows_b, c].astype(F32)
        )
        stats[z, pl.ds(b, 1), :] = sq
        stats[z, pl.ds(8 + b, 1), :] = inner

    mark("rows_wait")

    for n in range(len(offsets)):
        row_copy(n, True).wait()

    mark("embed")

    @pl.loop(0, N_CTX, unroll=4)
    def _(s):
        four = rows_in[s].astype(F32)
        for k in range(4):
            incf[pl.ds(k * N_CTX + s, 1), :] = four[k : k + 1, :]

    mark("new_sums")
    sq_new, inner_new = row_sums(lambda c: incf[:, c], lambda c: cotsel[:, c])
    sq_new = jnp.broadcast_to(sq_new, (SLOTS, SLOTS)).T
    inner_new = jnp.broadcast_to(inner_new, (SLOTS, SLOTS)).T
    for b in range(8):
        here = at_col == iota((SLOTS, SLOTS), 1) + 128 * b
        taken = jnp.sum(jnp.where(here, 1.0, 0.0), axis=0, keepdims=True) > 0.0
        for base, new in ((b, sq_new), (8 + b, inner_new)):
            put = jnp.sum(jnp.where(here, new, 0.0), axis=0, keepdims=True)
            stats[z, base : base + 1, :] = jnp.where(taken, put, stats[z, base : base + 1, :])

    def stat_copy(d, slot):
        return remote(
            stats.at[z], stats.at[slot], st_ss.at[d], st_rs.at[d], {"ctx": ctx, "tp": (z + d) % NZ}
        )

    mark("stat")

    @pl.loop(1, NZ)
    def _(d):
        stat_copy(d, z).start()

    mark("place")
    inc = incf[...].astype(BF16)

    @pl.loop(0, 8)
    def _(b):
        rows_b = pl.ds(pl.multiple_of(b * 128, 128), 128)
        placed = jnp.where(iota((128, SLOTS), 0) + 128 * b == at_row, 1.0, 0.0).astype(F32)
        taken = jnp.sum(placed, axis=1, keepdims=True) > 0.0
        vision = dot(placed.astype(BF16), inc)
        for n in range(8):
            cols_n = slice(128 * n, 128 * (n + 1))
            text[rows_b, cols_n] = jnp.where(taken, vision[:, cols_n].astype(BF16), text[rows_b, cols_n])

    def col_region(r, part):
        if part is None:
            return colin.at[pl.ds(r * 640, 640), :]
        return colin.at[pl.ds(r * 640 + part * 320, 320), :]

    cg = Ring(p, col_region, cg_ss, cg_rs)

    def turn_cols(r):
        @pl.loop(0, 4)
        def _(x):
            for h, ref in ((0, colf), (1, colg)):
                rows_s = pl.ds(pl.multiple_of(source((z + 2 * NZ - r - 2 * h) % NZ, x) * PITCH, 8), SLOTS)
                came = colin[pl.ds(pl.multiple_of(r * 640 + (h * 4 + x) * 80, 16), 80), :].astype(F32)
                ref[rows_s, :] = jnp.concatenate([came, jnp.zeros((48, 128), F32)], axis=0).T

    mark("col_wait")
    for h in range(2):
        for x in range(4):

            @pl.when(ctx != source((z + NZ - 2 * h) % NZ, x))
            def _():
                src, dst = half_block(0, h * 4 + x)
                remote(src, dst, co_ss.at[0], co_rs.at[h * 4 + x], {"ctx": p.sib, "tp": z}).wait_recv()

    cg.step(1)
    mark("stat_wait")

    @pl.loop(1, NZ)
    def _(d):
        stat_copy(d, (z + NZ - d) % NZ).wait()

    mark("drows")
    total = jnp.sum(stats[...], axis=0)
    scale = lax.rsqrt(total[0:8, :] / D + 1e-06)
    inner_all = total[8:16, :]
    scale_at = jnp.zeros((1, SLOTS), F32)
    inner_at = jnp.zeros((1, SLOTS), F32)
    for b in range(8):
        here = iota((128, SLOTS), 0) + 128 * b == at_row
        scale_b = jnp.broadcast_to(scale[b : b + 1, :], (128, 128)).T
        inner_b = jnp.broadcast_to(inner_all[b : b + 1, :], (128, 128)).T
        scol[128 * b : 128 * (b + 1), :] = scale_b
        scale_at = scale_at + jnp.sum(jnp.where(here, scale_b, 0.0), axis=0, keepdims=True)
        inner_at = inner_at + jnp.sum(jnp.where(here, inner_b, 0.0), axis=0, keepdims=True)
    s_at = jnp.broadcast_to(scale_at, (SLOTS, SLOTS)).T
    i_at = jnp.broadcast_to(inner_at, (SLOTS, SLOTS)).T
    own_g = pl.ds(pl.multiple_of(ctx * SLOTS, 128), SLOTS)
    for n in range(8):
        cols_n = slice(128 * n, 128 * (n + 1))
        gained = gain_of(n) * cotsel[:, cols_n]
        gf[own_g, cols_n] = (s_at * gained - incf[:, cols_n] * (s_at * s_at * s_at) * i_at / D).astype(BF16)

    gg = PlaneGather(p, gf, SLOTS, g_ss, g_rs)
    gg.start()

    def normed_copy(b):
        rows_b = pl.ds(pl.multiple_of(b * 256, 256), 256)
        return pltpu.make_async_copy(normed.at[rows_b, :], normed_out.at[rows_b, :], local.at[4 + b])

    def normed_block(b):
        for h in range(2):
            rows_b = pl.ds(b * 256 + h * 128, 128)
            for n in range(8):
                cols_n = slice(128 * n, 128 * (n + 1))
                normed[rows_b, cols_n] = (
                    text[rows_b, cols_n].astype(F32) * scol[rows_b, :] * gain_of(n)
                ).astype(BF16)
        normed_copy(b).start()

    def order_block(t):
        for k in range(4):
            rows_k = pl.ds(pl.multiple_of(t * SLOTS + k * N_CTX, 32), N_CTX)
            every = pl.ds(t * 4 + k, N_CTX, stride=PITCH)
            cols[rows_k, 0:80] = colf[every, :][:, 0:80].astype(BF16)
            cols[rows_k, 80:160] = colg[every, :][:, 0:80].astype(BF16)

    def add_pair(i, j, first=False):
        base = gg.pair_rows(i, j)
        rows_p = pl.ds(pl.multiple_of(base, 256), 256)
        part = lax.dot_general(
            cols[rows_p, :], gf[rows_p, :], (((0,), (0,)), ((), ())), preferred_element_type=F32
        )
        grad_out[...] = part if first else grad_out[...] + part

    def pair(i, j, first=False):
        base = gg.pair_rows(i, j) // SLOTS
        for h in range(2):
            order_block(base + h)
        gg.from_sibling(i, j)
        add_pair(i, j, first)

    mark("normed")
    normed_block(0)
    normed_block(1)
    normed_block(2)
    normed_block(3)
    turn_cols(0)
    mark("c1")
    cg.recv(1)
    cg.step(2)
    mark("col_t")
    turn_cols(1)
    turn_cols(7)
    mark("g1")
    gg.first()
    mark("g30")
    gg.third(0)
    mark("c2")
    cg.recv(2)
    cg.step(3)
    mark("col_t")
    turn_cols(2)
    turn_cols(6)
    mark("g2")
    gg.second()
    mark("g31")
    gg.third(1)
    mark("c3")
    cg.recv(3)
    cg.step(4)
    mark("col_t")
    turn_cols(3)
    turn_cols(5)
    mark("g32")
    gg.third(2)
    mark("c4")
    cg.recv(4)
    mark("col_t")
    turn_cols(4)
    mark("add0")
    pair(0, 0, True)
    pair(1, 0)
    pair(0, 1)
    mark("g33")
    gg.third(3)
    mark("add1")
    pair(2, 0)
    pair(0, 2)
    pair(1, 1)
    mark("g40")
    gg.fourth(0)
    mark("add2")
    pair(1, 2)
    pair(2, 1)
    pair(2, 2)
    mark("g41")
    gg.fourth(1)
    mark("add3")
    pair(3, 0)
    pair(0, 3)
    mark("g42")
    gg.fourth(2)
    mark("add4")
    pair(3, 1)
    pair(1, 3)
    mark("g43")
    gg.fourth(3)
    mark("add5")
    pair(3, 2)
    pair(2, 3)
    pair(3, 3)
    mark("end")
    for b in range(4):
        normed_copy(b).wait()
    for c in (wg, gg, og, ag, cg):
        c.finish()
    for c in osib:
        c.wait_send()

    @pl.when(turn)
    def _():
        for n in range(len(offsets)):
            col_copy(n).wait_send()

    mark(None)


def hand_out(normed_in, grad_in, normed_out, grad_out, normed, grad, sem_in, sem_out):
    parts = [
        (normed_in.at[pl.ds(r, 128), :], normed.at[pl.ds(r, 128), :], normed_out.at[pl.ds(r, 128), :])
        for r in range(0, TOK, 128)
    ] + [(grad_in, grad, grad_out)]
    come = [pltpu.make_async_copy(a, b, sem_in.at[n]) for n, (a, b, _) in enumerate(parts)]
    go = [pltpu.make_async_copy(b, c, sem_out.at[n]) for n, (_, b, c) in enumerate(parts)]
    for c in come:
        c.start()
    for c, g in zip(come, go):
        c.wait()
        g.start()
    for g in go:
        g.wait()


def shards(
    patches,
    window_ids,
    positions,
    text_embed,
    cotangent,
    qkv_weight,
    out_weight,
    merger_weight,
    norm_gain,
):
    vmem = pl.BlockSpec(memory_space=pltpu.VMEM)
    anywhere = pl.BlockSpec(memory_space=pl.ANY)
    dma = pltpu.SemaphoreType.DMA
    outs = pl.pallas_call(
        kernel,
        out_shape=(
            jax.ShapeDtypeStruct((TOK, 1024), BF16),
            jax.ShapeDtypeStruct((ROWS_W, 1024), F32),
        ),
        in_specs=[anywhere, vmem, vmem, anywhere, anywhere, anywhere, anywhere, anywhere, vmem],
        out_specs=(anywhere, vmem),
        scratch_shapes=[
            pltpu.VMEM((512, DV), BF16),
            pltpu.VMEM((3, HCOLS, DV), BF16),
            pltpu.VMEM((N_CTX * ROWS_W, 1024), BF16),
            pltpu.VMEM((N_CTX * SLOTS, 1024), BF16),
            pltpu.VMEM((DV, DV), BF16),
            pltpu.VMEM((DV, 512), BF16),
            pltpu.VMEM((512, 5 * HCOLS), BF16),
            pltpu.VMEM((512, 3 * HCOLS), BF16),
            pltpu.VMEM((512, DV), F32),
            pltpu.VMEM((512, DV), BF16),
            pltpu.VMEM((SLOTS, 4 * DV), BF16),
            pltpu.VMEM((4 * DV, SLOTS), BF16),
            pltpu.VMEM((N_CTX * ROWS_W, SLOTS), BF16),
            pltpu.VMEM((N_CTX * PITCH, 128), F32),
            pltpu.VMEM((N_CTX * PITCH, 128), F32),
            pltpu.VMEM((N_CTX * SLOTS, ROWS_W), BF16),
            pltpu.VMEM((TOK, 1024), BF16),
            pltpu.VMEM((TOK, 1024), BF16),
            pltpu.VMEM((TOK, 1024), BF16),
            pltpu.VMEM((512, HCOLS), BF16),
            pltpu.VMEM((512, HCOLS), BF16),
            pltpu.VMEM((512, HCOLS), BF16),
            pltpu.VMEM((HCOLS, 512), BF16),
            pltpu.VMEM((512, 128), jnp.int32),
            pltpu.VMEM((SLOTS, 1024), F32),
            pltpu.VMEM((N_CTX, 4, 1024), BF16),
            pltpu.VMEM((N_CTX, 4, 1024), BF16),
            pltpu.VMEM((SLOTS, 1024), F32),
            pltpu.VMEM((N_CTX, 8, SLOTS), jnp.int32),
            pltpu.VMEM((N_CTX, 8, SLOTS), jnp.int32),
            pltpu.VMEM((NZ, 16, SLOTS), F32),
            pltpu.VMEM((SLOTS, 1024), F32),
            pltpu.VMEM((TOK, SLOTS), F32),
            pltpu.VMEM((SLOTS, TOK), BF16),
            dma((10,)),
            dma((36,)), dma((36,)), dma((36,)), dma((36,)),
            dma((8,)), dma((8,)), dma((8,)), dma((8,)), dma((8,)), dma((8,)),
            dma((N_CTX,)), dma((N_CTX,)), dma((N_CTX,)), dma((N_CTX,)), dma((N_CTX,)), dma((8,)), dma((8,)), dma((8,)),
            dma((NZ,)), dma((NZ,)),
        ],
        compiler_params=pltpu.CompilerParams(
            collective_id=0, has_side_effects=True, vmem_limit_bytes=62 * 1024 * 1024
        ),
    )(
        patches,
        window_ids.reshape(1, -1),
        positions.reshape(1, -1),
        text_embed,
        cotangent,
        jnp.swapaxes(qkv_weight, 1, 2),
        out_weight,
        merger_weight,
        norm_gain.reshape(8, 128),
    )
    return pl.pallas_call(
        hand_out,
        out_shape=(
            jax.ShapeDtypeStruct((TOK, 1024), BF16),
            jax.ShapeDtypeStruct((ROWS_W, 1024), F32),
        ),
        in_specs=[anywhere, anywhere],
        out_specs=(anywhere, anywhere),
        scratch_shapes=[
            pltpu.VMEM((TOK, 1024), BF16),
            pltpu.VMEM((ROWS_W, 1024), F32),
            dma((9,)),
            dma((9,)),
        ],
    )(*outs)


def solution(mesh):
    in_specs = (
        P("ctx", None),
        P("ctx"),
        P("ctx"),
        P("ctx", "tp"),
        P("ctx", "tp"),
        P(None, None, "tp"),
        P("tp", None),
        P("ctx", "tp"),
        P("tp"),
    )
    out_specs = (P("ctx", "tp"), P("ctx", "tp"))
    return jax.shard_map(shards, mesh=mesh, in_specs=in_specs, out_specs=out_specs, check_vma=False)
```

```python
import jax
import jax.numpy as jnp
from jax import lax
from jax.experimental import pallas as pl
from jax.experimental.pallas import tpu as pltpu
from jax.sharding import PartitionSpec as P

MESH = pl.DeviceIdType.MESH
D = 8192
HEAD_DIM = 80
NX, NY, NC, NZ = 4, 4, 2, 8
N_CTX = 32
SLOTS = 128
TOK = 1024
DV = 1280
HCOLS = 160
ROWS_W = 160
PITCH = 136
F32 = jnp.float32
BF16 = jnp.bfloat16


def remote(src, dst, send, recv, dev):
    return pltpu.make_async_remote_copy(
        src_ref=src, dst_ref=dst, send_sem=send, recv_sem=recv, device_id=dev, device_id_type=MESH
    )


def dot(a, b):
    return jnp.dot(a, b, preferred_element_type=F32)


def dot_nt(a, b):
    return lax.dot_general(a, b, (((1,), (1,)), ((), ())), preferred_element_type=F32)


def iota(shape, dim):
    return lax.broadcasted_iota(jnp.int32, shape, dim)


class Place:
    def __init__(self):
        self.ctx = lax.axis_index("ctx")
        self.z = lax.axis_index("tp")
        self.core = self.ctx % 2
        y = (self.ctx // 2) % NY
        x = self.ctx // (2 * NY)
        self.f = x * (1 - self.core) + y * self.core
        self.g = y * (1 - self.core) + x * self.core
        self.sib = self.ctx + 1 - 2 * self.core
        self.offs = (0, 3, 1, 2)

    def ctx_of(self, f, g):
        x = f * (1 - self.core) + g * self.core
        y = g * (1 - self.core) + f * self.core
        return (x * NY + y) * 2 + self.core

    def near(self, df, dg):
        return self.ctx_of((self.f + df) % 4, (self.g + dg) % 4)

    def dev(self, df, dg):
        return {"ctx": self.near(df, dg), "tp": self.z}


class PlaneGather:
    def __init__(self, place, buf, rows, ss, rs, part):
        self.p, self.buf, self.rows, self.half = place, buf, rows, rows // 2
        self.ss, self.rs = ss.at[part], rs.at[part]
        self.lanes = pl.ds(part * 512, 512)
        self.started = []

    def block(self, df, dg, part=None):
        base = self.p.near(df, dg) * self.rows
        if part is None:
            return self.buf.at[pl.ds(pl.multiple_of(base, 32), self.rows), self.lanes]
        base = base + part * self.half
        return self.buf.at[pl.ds(pl.multiple_of(base, 16), self.half), self.lanes]

    def send(self, n, region, dev):
        c = remote(region, region, self.ss.at[n], self.rs.at[n], dev)
        c.start()
        self.started.append(c)

    def recv(self, n, region):
        remote(region, region, self.ss.at[n], self.rs.at[n], self.p.dev(0, 1)).wait_recv()

    def sibling(self, i, j):
        o = self.p.offs
        self.send(20 + 4 * i + j, self.block(o[i], o[j]), {"ctx": self.p.sib, "tp": self.p.z})

    def item(self, i):
        o = self.p.offs
        if i:
            self.sibling(i, 0)
        self.send(4 + 4 * i, self.block(o[i], 0), self.p.dev(0, 1))
        self.send(5 + 4 * i, self.block(o[i], 0), self.p.dev(0, 3))

    def start(self):
        own = self.block(0, 0)
        self.send(0, own, self.p.dev(1, 0))
        self.send(1, own, self.p.dev(3, 0))
        self.item(0)
        self.sibling(0, 0)

    def first(self):
        self.recv(0, self.block(3, 0))
        self.send(2, self.block(3, 0, 0), self.p.dev(1, 0))
        self.item(1)
        self.recv(1, self.block(1, 0))
        self.send(3, self.block(1, 0, 1), self.p.dev(3, 0))
        self.item(2)

    def second(self):
        self.recv(2, self.block(2, 0, 0))
        self.recv(3, self.block(2, 0, 1))
        self.item(3)

    def third(self, i):
        o = self.p.offs[i]
        self.recv(4 + 4 * i, self.block(o, 3))
        self.send(6 + 4 * i, self.block(o, 3, 0), self.p.dev(0, 1))
        self.sibling(i, 1)
        self.recv(5 + 4 * i, self.block(o, 1))
        self.send(7 + 4 * i, self.block(o, 1, 1), self.p.dev(0, 3))
        self.sibling(i, 2)

    def fourth(self, i):
        o = self.p.offs[i]
        self.recv(6 + 4 * i, self.block(o, 2, 0))
        self.recv(7 + 4 * i, self.block(o, 2, 1))
        self.sibling(i, 3)

    def from_sibling(self, i, j):
        o = self.p.offs
        base = self.p.near(o[i], o[j]) + 1 - 2 * self.p.core
        region = self.buf.at[pl.ds(pl.multiple_of(base * self.rows, 32), self.rows), self.lanes]
        self.recv(20 + 4 * j + i, region)

    def pair_rows(self, i, j):
        o = self.p.offs
        return (self.p.near(o[i], o[j]) - self.p.core) * self.rows

    def finish(self):
        for c in self.started:
            c.wait_send()


class Ring:
    def __init__(self, place, region, ss, rs):
        self.p, self.region, self.ss, self.rs = place, region, ss, rs
        self.started = []

    def copy(self, s, way):
        part = way if s == 4 else None
        src = (s - 1, (NZ + 1 - s) % NZ)[way]
        dst = (s, NZ - s)[way]
        return remote(
            self.region(src, part), self.region(dst, part), self.ss.at[4 * way + s - 1], self.rs.at[4 * way + s - 1],
            {"ctx": self.p.ctx, "tp": (self.p.z + (1, NZ - 1)[way]) % NZ},
        )

    def step(self, s):
        for way in range(2):
            c = self.copy(s, way)
            c.start()
            self.started.append(c)

    def recv(self, s):
        for way in range(2):
            self.copy(s, way).wait_recv()

    def finish(self):
        for c in self.started:
            c.wait_send()


def kernel(
    pat_in, wid, pos, text_in, cot_in, qkv_in, ow_in, w_in, gain,
    normed, grad_out,
    pat, qkv, wf, gf, owf, attf, att_t, att_u, att_v, hacc, hid, perm, colsend, colin, colf, colg, cols, text, cot,
    q0s, q1s, ks, vts, widc, mrow, rows_send, rows_in, incf, idx_send, idx_in, stats, cotsel, scol, drow,
    local, w_ss, w_rs, g_ss, g_rs, ow_ss, ow_rs, osib_ss, osib_rs, at_ss, at_rs,
    ix_ss, ix_rs, rw_ss, rw_rs, co_ss, co_rs, cg_ss, cg_rs, st_ss, st_rs,
):
    p = Place()
    ctx, z, core = p.ctx, p.z, p.core

    def other(d):
        return (ctx + d) % N_CTX

    def behind(d):
        return (ctx + N_CTX - d) % N_CTX

    scope = []

    def mark(name):
        if scope:
            scope.pop().__exit__(None, None, None)
        if name:
            scope.append(jax.named_scope(name))
            scope[-1].__enter__()

    mark("index")
    load_pat = pltpu.make_async_copy(pat_in, pat, local.at[8])
    load_qkv = pltpu.make_async_copy(qkv_in, qkv, local.at[9])
    load_pat.start()
    load_qkv.start()

    def block160(ref, c):
        return ref.at[pl.ds(pl.multiple_of(c * ROWS_W, 32), ROWS_W), :]

    barrier = pltpu.get_barrier_semaphore()

    @pl.loop(1, N_CTX)
    def _(d):
        pl.semaphore_signal(barrier, inc=1, device_id={"ctx": other(d), "tp": z}, device_id_type=MESH)

    @pl.loop(1, NZ)
    def _(d):
        pl.semaphore_signal(barrier, inc=1, device_id={"ctx": ctx, "tp": (z + d) % NZ}, device_id_type=MESH)

    own_w = wf.at[pl.ds(pl.multiple_of(ctx * ROWS_W, 32), ROWS_W), :]
    own_ow = owf.at[pl.ds(0, HCOLS), :]
    load_w = pltpu.make_async_copy(w_in, own_w, local.at[0])
    load_ow = pltpu.make_async_copy(ow_in, own_ow, local.at[1])
    load_text = pltpu.make_async_copy(text_in, text, local.at[2])
    load_cot = pltpu.make_async_copy(cot_in, cot, local.at[3])
    load_w.start()
    load_ow.start()
    load_text.start()
    load_cot.start()

    pos_row = pos[...]
    pos_col = jnp.broadcast_to(pos_row, (SLOTS, SLOTS)).T
    t_row = pos_row // TOK
    t_col = pos_col // TOK
    same = t_col == t_row
    earlier_down = same & (iota((SLOTS, SLOTS), 0) < iota((SLOTS, SLOTS), 1))
    earlier_across = same & (iota((SLOTS, SLOTS), 1) < iota((SLOTS, SLOTS), 0))
    rank_row = jnp.sum(jnp.where(earlier_down, 1.0, 0.0).astype(F32), axis=0, keepdims=True)
    rank_col = jnp.sum(jnp.where(earlier_across, 1.0, 0.0).astype(F32), axis=1, keepdims=True)
    live_row = t_row < N_CTX
    bucket_row = jnp.where(live_row, t_row.astype(F32) * 4.0 + rank_row, -1.0)
    to_owner = jnp.where(iota((N_CTX, SLOTS), 0) == t_row, 1.0, 0.0).astype(BF16)
    row_no = pos_col % TOK + 1
    lane_of = rank_col.astype(jnp.int32) * N_CTX + ctx
    at_lane = lane_of == iota((SLOTS, SLOTS), 1)
    high = jnp.where(at_lane, (row_no // 32).astype(F32), 0.0).astype(BF16)
    low = jnp.where(at_lane, (row_no % 32).astype(F32), 0.0).astype(BF16)
    index_rows = (dot(to_owner, high) * 32.0 + dot(to_owner, low)).astype(jnp.int32)
    for t in range(N_CTX):
        idx_send[t] = jnp.broadcast_to(index_rows[t : t + 1, :], (8, SLOTS))
    idx_in[ctx] = idx_send[ctx]

    for b in range(4):
        widc[128 * b : 128 * (b + 1), :] = jnp.broadcast_to(wid[:, 128 * b : 128 * (b + 1)], (128, 128)).T

    mark("qkv")
    load_pat.wait()
    load_qkv.wait()
    patches = pat[...]
    lane = iota((512, HCOLS), 1)
    q = dot_nt(patches, qkv[0]).astype(BF16).astype(F32)
    q0s[...] = jnp.where(lane < HEAD_DIM, q, 0.0).astype(BF16)
    q1s[...] = jnp.where(lane < HEAD_DIM, 0.0, q).astype(BF16)
    ks[...] = dot_nt(patches, qkv[1]).astype(BF16)
    vts[...] = dot_nt(qkv[2], patches).astype(BF16)
    mark("barrier")
    pl.semaphore_wait(barrier, N_CTX - 1 + NZ - 1)

    w0, w1 = (PlaneGather(p, wf, ROWS_W, w_ss, w_rs, n) for n in range(2))
    load_w.wait()
    w0.start()
    w1.start()

    def place_of(r):
        return (0, 1, 7, 2, 6, 3, 5, 4).index(r)

    def ow_region(r, part):
        base = pl.multiple_of(place_of(r) * HCOLS + core * 80, 16)
        if part is None:
            return owf.at[pl.ds(base, 80), :]
        return owf.at[pl.ds(base, 80), pl.ds(part * 640, 640)]

    def att_region(r, part):
        if part is None:
            return attf.at[pl.ds(place_of(r) * HCOLS, HCOLS), :]
        return attf.at[pl.ds(place_of(r) * HCOLS + part * 80, 80), :]

    osib = []

    def ow_to_sibling(r):
        src = ow_region(r, None)
        c = remote(src, src, osib_ss.at[r], osib_rs.at[r], {"ctx": p.sib, "tp": z})
        c.start()
        osib.append(c)

    def ow_from_sibling(r):
        dst = owf.at[pl.ds(pl.multiple_of(place_of(r) * HCOLS + (1 - core) * 80, 16), 80), :]
        remote(dst, dst, osib_ss.at[r], osib_rs.at[r], {"ctx": p.sib, "tp": z}).wait_recv()

    og = Ring(p, ow_region, ow_ss, ow_rs)
    ag = Ring(p, att_region, at_ss, at_rs)
    load_ow.wait()
    og.step(1)
    mark("attend")
    factor = 1.0 / HEAD_DIM**0.5

    @pl.loop(0, 4)
    def _(b):
        cols_b = pl.ds(pl.multiple_of(b * 128, 128), 128)
        ids = wid[:, cols_b]
        allowed = (widc[...] == ids) & (widc[...] >= 0)
        parts = []
        for qs in (q0s, q1s):
            scores = dot_nt(ks[...], qs[cols_b, :]) * factor
            scores = jnp.where(allowed, scores, -1e30)
            weights = jnp.exp(scores - jnp.max(scores, axis=0, keepdims=True))
            probs = (weights / jnp.sum(weights, axis=0, keepdims=True)).astype(BF16)
            parts.append(dot(vts[...], probs))
        row = iota((HCOLS, 128), 0)
        attf[0:HCOLS, cols_b] = jnp.where(
            row < HEAD_DIM, parts[0], parts[1]
        ).astype(BF16)

    ag.step(1)

    def turn_att(r):
        k = place_of(r)
        part = attf[k * HCOLS : (k + 1) * HCOLS, :].T
        if k < 5:
            att_t[:, k * HCOLS : (k + 1) * HCOLS] = part
        elif k < 7:
            att_u[:, (k - 5) * HCOLS : (k - 4) * HCOLS] = part
        else:
            att_v[...] = part

    def near_product(n):
        cols_n = slice(n * 256, (n + 1) * 256)
        hacc[:, cols_n] = pat[:, cols_n].astype(F32) + dot(att_t[...], owf[0 : 5 * HCOLS, cols_n])

    def middle_product(n):
        cols_n = slice(n * 256, (n + 1) * 256)
        hacc[:, cols_n] += dot(att_u[:, 0 : 2 * HCOLS], owf[5 * HCOLS : 7 * HCOLS, cols_n])

    turn_att(0)
    mark("w_first0")
    w0.first()
    w0.third(0)
    mark("ow1")
    og.recv(1)
    og.step(2)
    ow_to_sibling(1)
    ow_to_sibling(7)
    mark("w_first1")
    w1.first()
    w1.third(0)
    mark("at1")
    ag.recv(1)
    ag.step(2)
    turn_att(1)
    turn_att(7)

    @pl.loop(1, N_CTX)
    def _(d):
        remote(
            idx_send.at[other(d)], idx_in.at[ctx], ix_ss.at[d], ix_rs.at[d], {"ctx": other(d), "tp": z}
        ).start()

    mark("w_second0")
    w0.second()
    mark("w31_0")
    w0.third(1)
    mark("w_second1")
    w1.second()
    mark("ow2")
    og.recv(2)
    og.step(3)
    ow_to_sibling(2)
    ow_to_sibling(6)
    mark("w32_0")
    w0.third(2)
    mark("w31_1")
    w1.third(1)
    mark("at2")
    ag.recv(2)
    ag.step(3)
    turn_att(2)
    turn_att(6)
    for r in (1, 7, 2, 6):
        ow_from_sibling(r)
    near_product(0)
    mark("w32_1")
    w1.third(2)
    near_product(1)
    mark("w33_0")
    w0.third(3)
    mark("ow3")
    og.recv(3)
    og.step(4)
    ow_to_sibling(3)
    ow_to_sibling(5)
    near_product(2)
    mark("w33_1")
    w1.third(3)
    mark("w40_0")
    w0.fourth(0)
    w0.fourth(1)
    near_product(3)
    mark("at3")
    ag.recv(3)
    ag.step(4)
    turn_att(3)
    turn_att(5)
    mark("w40_1")
    w1.fourth(0)
    w1.fourth(1)
    near_product(4)
    for r in (3, 5):
        ow_from_sibling(r)
    middle_product(0)
    middle_product(1)
    mark("ow4")
    og.recv(4)
    ow_to_sibling(4)
    middle_product(2)
    mark("w42_0")
    w0.fourth(2)
    w0.fourth(3)
    middle_product(3)
    middle_product(4)
    mark("at4")
    ag.recv(4)
    ow_from_sibling(4)
    mark("w42_1")
    w1.fourth(2)
    w1.fourth(3)
    mark("hidden")
    turn_att(4)

    @pl.loop(0, 5)
    def _(n):
        cols_n = pl.ds(pl.multiple_of(n * 256, 256), 256)
        hid[:, cols_n] = (hacc[:, cols_n] + dot(att_v[...], owf[7 * HCOLS : 8 * HCOLS, cols_n])).astype(BF16)

    mark("perm")
    spread_at = jnp.where(iota((SLOTS, 512), 0) == iota((SLOTS, 512), 1) // 4, 1.0, 0.0).astype(BF16)
    bucket512 = dot(jnp.broadcast_to(bucket_row, (8, SLOTS)).astype(BF16), spread_at)[0:1, :]
    chosen = iota((SLOTS, 512), 0).astype(F32) == bucket512
    for i in range(4):
        select = jnp.where(chosen & (iota((SLOTS, 512), 1) % 4 == i), 1.0, 0.0).astype(BF16)
        for n in range(5):
            perm[:, i * DV + n * 256 : i * DV + (n + 1) * 256] = dot(
                select, hid[:, n * 256 : (n + 1) * 256]
            ).astype(BF16)

    def at_offset(dx, dy, dc):
        x = (ctx // (2 * NY) + dx) % NX
        y = ((ctx // 2) % NY + dy) % NY
        return (x * NY + y) * 2 + (core + dc) % 2

    hops = (0, 1, 2, 1)
    offsets = sorted(
        ((dx, dy, dc) for dx in range(4) for dy in range(4) for dc in range(2) if dx + dy + dc > 0),
        key=lambda o: (-hops[o[0]] - hops[o[1]], o),
    )

    def row_copy(n, part, arriving):
        dx, dy, dc = offsets[n]
        to = at_offset(dx, dy, dc)
        slot = at_offset(-dx % 4, -dy % 4, dc) if arriving else ctx
        lanes = pl.ds(part * 512, 512)
        return remote(
            rows_send.at[to, :, lanes], rows_in.at[slot, :, lanes], rw_ss.at[part, n], rw_rs.at[part, n],
            {"ctx": to, "tp": z},
        )

    for part, w in ((0, w0), (1, w1)):
        mark("w_sib")
        for i in range(4):
            for j in range(4):
                w.from_sibling(i, j)
        mark("merge")
        for n in (2 * part, 2 * part + 1):
            cols_n = slice(256 * n, 256 * (n + 1))
            mrow[:, cols_n] = dot(perm[...], wf[:, cols_n]).astype(BF16).astype(F32)
        lanes = slice(512 * part, 512 * (part + 1))

        @pl.loop(0, N_CTX // 2, unroll=4)
        def _(t):
            eight = mrow[pl.ds(pl.multiple_of(t * 8, 8), 8), lanes]
            rows_send[2 * t, :, lanes] = eight[0:4, :].astype(BF16)
            rows_send[2 * t + 1, :, lanes] = eight[4:8, :].astype(BF16)

        for n in range(len(offsets)):
            row_copy(n, part, False).start()

    rows_in[ctx] = rows_send[ctx]

    mark("colsend")

    def source(zz, x):
        return (x * NY + (x + zz) % NY) * 2 + zz // NY

    x_here = ctx // (2 * NY)
    plane = (z - ((ctx // 2) % NY - x_here + NY) % NY - NY * core + NZ) % NZ
    turn = (plane == 0) | (plane == 2)
    half = plane // 2

    def half_block(c, slot):
        return (
            colsend.at[pl.ds(pl.multiple_of(c * ROWS_W + (half % 2) * 80, 16), 80), :],
            colin.at[pl.ds(pl.multiple_of(slot * 80, 16), 80), :],
        )

    def col_copy(n):
        to = at_offset(*offsets[n])
        slot = (half % 2) * 4 + x_here
        src, dst = half_block(to, slot)
        return remote(src, dst, co_ss.at[n], co_rs.at[slot], {"ctx": to, "tp": z})

    @pl.when(turn)
    def _():
        for n in range(40):
            colsend[n * 128 : (n + 1) * 128, :] = perm[:, n * 128 : (n + 1) * 128].T

        for n in range(len(offsets)):
            col_copy(n).start()
        mine = pl.ds(pl.multiple_of(ctx * ROWS_W + (half % 2) * 80, 16), 80)
        colin[pl.ds(pl.multiple_of(((half % 2) * 4 + x_here) * 80, 16), 80), :] = colsend[mine, :]

    mark("idx_wait")
    @pl.loop(1, N_CTX)
    def _(d):
        remote(
            idx_send.at[other(d)], idx_in.at[behind(d)], ix_ss.at[d], ix_rs.at[d], {"ctx": other(d), "tp": z}
        ).wait()

    mark("cotsel")
    load_text.wait()
    load_cot.wait()
    at_row = (jnp.sum(idx_in[...], axis=0) - 1)[0:1, :]
    at_col = jnp.broadcast_to(at_row, (SLOTS, SLOTS)).T
    for b in range(8):
        drow[:, 128 * b : 128 * (b + 1)] = jnp.where(
            at_col == iota((SLOTS, SLOTS), 1) + 128 * b, 1.0, 0.0
        ).astype(BF16)

    @pl.loop(0, 4)
    def _(n):
        cols_n = pl.ds(pl.multiple_of(n * 256, 256), 256)
        cotsel[:, cols_n] = dot(drow[...], cot[:, cols_n])

    gains = gain[...].astype(F32)

    def gain_of(n):
        return gains[n : n + 1, :]

    def row_sums(rows, cots):
        sq = jnp.zeros((128, 128), F32)
        inner = jnp.zeros((128, 128), F32)
        for n in range(8):
            cols_n = slice(128 * n, 128 * (n + 1))
            x = rows(cols_n)
            sq = sq + x * x
            inner = inner + x * (gain_of(n) * cots(cols_n))
        return jnp.sum(sq.T, axis=0, keepdims=True), jnp.sum(inner.T, axis=0, keepdims=True)

    mark("text_sums")

    @pl.loop(0, 8)
    def _(b):
        rows_b = pl.ds(pl.multiple_of(b * 128, 128), 128)
        sq, inner = row_sums(
            lambda c: text[rows_b, c].astype(F32), lambda c: cot[rows_b, c].astype(F32)
        )
        stats[z, pl.ds(b, 1), :] = sq
        stats[z, pl.ds(8 + b, 1), :] = inner

    mark("rows_wait")

    for part in range(2):
        for n in range(len(offsets)):
            row_copy(n, part, True).wait()

    mark("embed")

    @pl.loop(0, N_CTX, unroll=4)
    def _(s):
        four = rows_in[s].astype(F32)
        for k in range(4):
            incf[pl.ds(k * N_CTX + s, 1), :] = four[k : k + 1, :]

    mark("new_sums")
    sq_new, inner_new = row_sums(lambda c: incf[:, c], lambda c: cotsel[:, c])
    sq_new = jnp.broadcast_to(sq_new, (SLOTS, SLOTS)).T
    inner_new = jnp.broadcast_to(inner_new, (SLOTS, SLOTS)).T
    for b in range(8):
        here = at_col == iota((SLOTS, SLOTS), 1) + 128 * b
        taken = jnp.sum(jnp.where(here, 1.0, 0.0), axis=0, keepdims=True) > 0.0
        for base, new in ((b, sq_new), (8 + b, inner_new)):
            put = jnp.sum(jnp.where(here, new, 0.0), axis=0, keepdims=True)
            stats[z, base : base + 1, :] = jnp.where(taken, put, stats[z, base : base + 1, :])

    def stat_copy(d, slot):
        return remote(
            stats.at[z], stats.at[slot], st_ss.at[d], st_rs.at[d], {"ctx": ctx, "tp": (z + d) % NZ}
        )

    mark("stat")

    @pl.loop(1, NZ)
    def _(d):
        stat_copy(d, z).start()

    mark("place")
    inc = incf[...].astype(BF16)

    @pl.loop(0, 8)
    def _(b):
        rows_b = pl.ds(pl.multiple_of(b * 128, 128), 128)
        placed = jnp.where(iota((128, SLOTS), 0) + 128 * b == at_row, 1.0, 0.0).astype(F32)
        taken = jnp.sum(placed, axis=1, keepdims=True) > 0.0
        vision = dot(placed.astype(BF16), inc)
        for n in range(8):
            cols_n = slice(128 * n, 128 * (n + 1))
            text[rows_b, cols_n] = jnp.where(taken, vision[:, cols_n].astype(BF16), text[rows_b, cols_n])

    def col_region(r, part):
        if part is None:
            return colin.at[pl.ds(r * 640, 640), :]
        return colin.at[pl.ds(r * 640 + part * 320, 320), :]

    cg = Ring(p, col_region, cg_ss, cg_rs)

    def turn_cols(r):
        @pl.loop(0, 4)
        def _(x):
            for h, ref in ((0, colf), (1, colg)):
                rows_s = pl.ds(pl.multiple_of(source((z + 2 * NZ - r - 2 * h) % NZ, x) * PITCH, 8), SLOTS)
                came = colin[pl.ds(pl.multiple_of(r * 640 + (h * 4 + x) * 80, 16), 80), :].astype(F32)
                ref[rows_s, :] = jnp.concatenate([came, jnp.zeros((48, 128), F32)], axis=0).T

    mark("col_wait")
    for h in range(2):
        for x in range(4):

            @pl.when(ctx != source((z + NZ - 2 * h) % NZ, x))
            def _():
                src, dst = half_block(0, h * 4 + x)
                remote(src, dst, co_ss.at[0], co_rs.at[h * 4 + x], {"ctx": p.sib, "tp": z}).wait_recv()

    cg.step(1)
    mark("stat_wait")

    @pl.loop(1, NZ)
    def _(d):
        stat_copy(d, (z + NZ - d) % NZ).wait()

    mark("drows")
    total = jnp.sum(stats[...], axis=0)
    scale = lax.rsqrt(total[0:8, :] / D + 1e-06)
    inner_all = total[8:16, :]
    scale_at = jnp.zeros((1, SLOTS), F32)
    inner_at = jnp.zeros((1, SLOTS), F32)
    for b in range(8):
        here = iota((128, SLOTS), 0) + 128 * b == at_row
        scale_b = jnp.broadcast_to(scale[b : b + 1, :], (128, 128)).T
        inner_b = jnp.broadcast_to(inner_all[b : b + 1, :], (128, 128)).T
        scol[128 * b : 128 * (b + 1), :] = scale_b
        scale_at = scale_at + jnp.sum(jnp.where(here, scale_b, 0.0), axis=0, keepdims=True)
        inner_at = inner_at + jnp.sum(jnp.where(here, inner_b, 0.0), axis=0, keepdims=True)
    s_at = jnp.broadcast_to(scale_at, (SLOTS, SLOTS)).T
    i_at = jnp.broadcast_to(inner_at, (SLOTS, SLOTS)).T
    own_g = pl.ds(pl.multiple_of(ctx * SLOTS, 128), SLOTS)
    for n in range(8):
        cols_n = slice(128 * n, 128 * (n + 1))
        gained = gain_of(n) * cotsel[:, cols_n]
        gf[own_g, cols_n] = (s_at * gained - incf[:, cols_n] * (s_at * s_at * s_at) * i_at / D).astype(BF16)

    g0, g1 = (PlaneGather(p, gf, SLOTS, g_ss, g_rs, n) for n in range(2))
    g0.start()
    g1.start()

    def normed_block(b):
        for h in range(2):
            rows_b = pl.ds(b * 256 + h * 128, 128)
            for n in range(8):
                cols_n = slice(128 * n, 128 * (n + 1))
                normed[rows_b, cols_n] = (
                    text[rows_b, cols_n].astype(F32) * scol[rows_b, :] * gain_of(n)
                ).astype(BF16)

    def order_block(t):
        for k in range(4):
            rows_k = pl.ds(pl.multiple_of(t * SLOTS + k * N_CTX, 32), N_CTX)
            every = pl.ds(t * 4 + k, N_CTX, stride=PITCH)
            cols[rows_k, 0:80] = colf[every, :][:, 0:80].astype(BF16)
            cols[rows_k, 80:160] = colg[every, :][:, 0:80].astype(BF16)

    def add_pair(i, j, first=False):
        base = g0.pair_rows(i, j)
        rows_p = pl.ds(pl.multiple_of(base, 256), 256)
        part = lax.dot_general(
            cols[rows_p, :], gf[rows_p, :], (((0,), (0,)), ((), ())), preferred_element_type=F32
        )
        grad_out[...] = part if first else grad_out[...] + part

    def pair(i, j, first=False):
        base = g0.pair_rows(i, j) // SLOTS
        for h in range(2):
            order_block(base + h)
        g0.from_sibling(i, j)
        g1.from_sibling(i, j)
        add_pair(i, j, first)

    mark("normed")
    normed_block(0)
    normed_block(1)
    normed_block(2)
    normed_block(3)
    turn_cols(0)
    mark("c1")
    cg.recv(1)
    cg.step(2)
    mark("g1_0")
    g0.first()
    g0.third(0)
    mark("col_t")
    turn_cols(1)
    turn_cols(7)
    mark("g1_1")
    g1.first()
    g1.third(0)
    mark("c2")
    cg.recv(2)
    cg.step(3)
    mark("g2_0")
    g0.second()
    mark("g31_0")
    g0.third(1)
    mark("col_t")
    turn_cols(2)
    turn_cols(6)
    mark("g2_1")
    g1.second()
    mark("g32_0")
    g0.third(2)
    mark("g31_1")
    g1.third(1)
    mark("c3")
    cg.recv(3)
    cg.step(4)
    mark("col_t")
    turn_cols(3)
    turn_cols(5)
    mark("g32_1")
    g1.third(2)
    mark("g33_0")
    g0.third(3)
    mark("c4")
    cg.recv(4)
    mark("g33_1")
    g1.third(3)
    mark("col_t")
    turn_cols(4)
    mark("add0")
    pair(0, 0, True)
    pair(1, 0)
    pair(0, 1)
    mark("g40_0")
    g0.fourth(0)
    g0.fourth(1)
    mark("add1")
    pair(2, 0)
    pair(0, 2)
    pair(1, 1)
    mark("g40_1")
    g1.fourth(0)
    g1.fourth(1)
    mark("add2")
    pair(1, 2)
    pair(2, 1)
    pair(2, 2)
    mark("g42_0")
    g0.fourth(2)
    mark("add3")
    pair(3, 0)
    pair(0, 3)
    mark("g42_1")
    g1.fourth(2)
    mark("g43_0")
    g0.fourth(3)
    mark("add4")
    pair(3, 1)
    pair(1, 3)
    mark("g43_1")
    g1.fourth(3)
    mark("add5")
    pair(3, 2)
    pair(2, 3)
    pair(3, 3)
    mark("end")
    for c in (w0, w1, g0, g1, og, ag, cg):
        c.finish()
    for c in osib:
        c.wait_send()

    @pl.when(turn)
    def _():
        for n in range(len(offsets)):
            col_copy(n).wait_send()

    mark(None)


def hand_out(normed, grad, normed_out, grad_out, sems):
    go = [
        pltpu.make_async_copy(normed, normed_out, sems.at[0]),
        pltpu.make_async_copy(grad, grad_out, sems.at[1]),
    ]
    for g in go:
        g.start()
    for g in go:
        g.wait()


def shards(
    patches,
    window_ids,
    positions,
    text_embed,
    cotangent,
    qkv_weight,
    out_weight,
    merger_weight,
    norm_gain,
):
    vmem = pl.BlockSpec(memory_space=pltpu.VMEM)
    anywhere = pl.BlockSpec(memory_space=pl.ANY)
    dma = pltpu.SemaphoreType.DMA
    outs = pl.pallas_call(
        kernel,
        out_shape=(pltpu.VMEM((TOK, 1024), BF16), pltpu.VMEM((ROWS_W, 1024), F32)),
        in_specs=[anywhere, vmem, vmem, anywhere, anywhere, anywhere, anywhere, anywhere, vmem],
        out_specs=(vmem, vmem),
        scratch_shapes=[
            pltpu.VMEM((512, DV), BF16),
            pltpu.VMEM((3, HCOLS, DV), BF16),
            pltpu.VMEM((N_CTX * ROWS_W, 1024), BF16),
            pltpu.VMEM((N_CTX * SLOTS, 1024), BF16),
            pltpu.VMEM((DV, DV), BF16),
            pltpu.VMEM((DV, 512), BF16),
            pltpu.VMEM((512, 5 * HCOLS), BF16),
            pltpu.VMEM((512, 2 * HCOLS), BF16),
            pltpu.VMEM((512, HCOLS), BF16),
            pltpu.VMEM((512, DV), F32),
            pltpu.VMEM((512, DV), BF16),
            pltpu.VMEM((SLOTS, 4 * DV), BF16),
            pltpu.VMEM((4 * DV, SLOTS), BF16),
            pltpu.VMEM((N_CTX * ROWS_W, SLOTS), BF16),
            pltpu.VMEM((N_CTX * PITCH, 128), F32),
            pltpu.VMEM((N_CTX * PITCH, 128), F32),
            pltpu.VMEM((N_CTX * SLOTS, ROWS_W), BF16),
            pltpu.VMEM((TOK, 1024), BF16),
            pltpu.VMEM((TOK, 1024), BF16),
            pltpu.VMEM((512, HCOLS), BF16),
            pltpu.VMEM((512, HCOLS), BF16),
            pltpu.VMEM((512, HCOLS), BF16),
            pltpu.VMEM((HCOLS, 512), BF16),
            pltpu.VMEM((512, 128), jnp.int32),
            pltpu.VMEM((SLOTS, 1024), F32),
            pltpu.VMEM((N_CTX, 4, 1024), BF16),
            pltpu.VMEM((N_CTX, 4, 1024), BF16),
            pltpu.VMEM((SLOTS, 1024), F32),
            pltpu.VMEM((N_CTX, 8, SLOTS), jnp.int32),
            pltpu.VMEM((N_CTX, 8, SLOTS), jnp.int32),
            pltpu.VMEM((NZ, 16, SLOTS), F32),
            pltpu.VMEM((SLOTS, 1024), F32),
            pltpu.VMEM((TOK, SLOTS), F32),
            pltpu.VMEM((SLOTS, TOK), BF16),
            dma((10,)),
            dma((2, 36)), dma((2, 36)), dma((2, 36)), dma((2, 36)),
            dma((8,)), dma((8,)), dma((8,)), dma((8,)), dma((8,)), dma((8,)),
            dma((N_CTX,)), dma((N_CTX,)), dma((2, N_CTX)), dma((2, N_CTX)), dma((N_CTX,)), dma((8,)), dma((8,)), dma((8,)),
            dma((NZ,)), dma((NZ,)),
        ],
        compiler_params=pltpu.CompilerParams(
            collective_id=0, has_side_effects=True, vmem_limit_bytes=56 * 1024 * 1024
        ),
    )(
        patches,
        window_ids.reshape(1, -1),
        positions.reshape(1, -1),
        text_embed,
        cotangent,
        jnp.swapaxes(qkv_weight, 1, 2),
        out_weight,
        merger_weight,
        norm_gain.reshape(8, 128),
    )
    return pl.pallas_call(
        hand_out,
        out_shape=(
            jax.ShapeDtypeStruct((TOK, 1024), BF16),
            jax.ShapeDtypeStruct((ROWS_W, 1024), F32),
        ),
        in_specs=[anywhere, anywhere],
        out_specs=(anywhere, anywhere),
        scratch_shapes=[
            dma((2,)),
        ],
        compiler_params=pltpu.CompilerParams(vmem_limit_bytes=1024 * 1024),
    )(*outs)


def solution(mesh):
    in_specs = (
        P("ctx", None),
        P("ctx"),
        P("ctx"),
        P("ctx", "tp"),
        P("ctx", "tp"),
        P(None, None, "tp"),
        P("tp", None),
        P("ctx", "tp"),
        P("tp"),
    )
    out_specs = (P("ctx", "tp"), P("ctx", "tp"))
    return jax.shard_map(shards, mesh=mesh, in_specs=in_specs, out_specs=out_specs, check_vma=False)
```

```python
import jax
import jax.numpy as jnp
from jax import lax
from jax.experimental import pallas as pl
from jax.experimental.pallas import tpu as pltpu
from jax.sharding import PartitionSpec as P

MESH = pl.DeviceIdType.MESH
D = 8192
HEAD_DIM = 80
NX, NY, NC, NZ = 4, 4, 2, 8
N_CTX = 32
SLOTS = 128
TOK = 1024
DV = 1280
HCOLS = 160
ROWS_W = 160
PITCH = 136
F32 = jnp.float32
BF16 = jnp.bfloat16


def remote(src, dst, send, recv, dev):
    return pltpu.make_async_remote_copy(
        src_ref=src, dst_ref=dst, send_sem=send, recv_sem=recv, device_id=dev, device_id_type=MESH
    )


def dot(a, b):
    return jnp.dot(a, b, preferred_element_type=F32)


def dot_nt(a, b):
    return lax.dot_general(a, b, (((1,), (1,)), ((), ())), preferred_element_type=F32)


def iota(shape, dim):
    return lax.broadcasted_iota(jnp.int32, shape, dim)


class Place:
    def __init__(self):
        self.ctx = lax.axis_index("ctx")
        self.z = lax.axis_index("tp")
        self.core = self.ctx % 2
        y = (self.ctx // 2) % NY
        x = self.ctx // (2 * NY)
        self.f = x * (1 - self.core) + y * self.core
        self.g = y * (1 - self.core) + x * self.core
        self.sib = self.ctx + 1 - 2 * self.core
        self.offs = (0, 3, 1, 2)

    def ctx_of(self, f, g):
        x = f * (1 - self.core) + g * self.core
        y = g * (1 - self.core) + f * self.core
        return (x * NY + y) * 2 + self.core

    def near(self, df, dg):
        return self.ctx_of((self.f + df) % 4, (self.g + dg) % 4)

    def dev(self, df, dg):
        return {"ctx": self.near(df, dg), "tp": self.z}


class PlaneGather:
    def __init__(self, place, buf, rows, ss, rs, part):
        self.p, self.buf, self.rows, self.half = place, buf, rows, rows // 2
        self.ss, self.rs = ss.at[part], rs.at[part]
        self.lanes = pl.ds(part * 512, 512)
        self.started = []

    def block(self, df, dg, part=None):
        base = self.p.near(df, dg) * self.rows
        if part is None:
            return self.buf.at[pl.ds(pl.multiple_of(base, 32), self.rows), self.lanes]
        base = base + part * self.half
        return self.buf.at[pl.ds(pl.multiple_of(base, 16), self.half), self.lanes]

    def send(self, n, region, dev):
        c = remote(region, region, self.ss.at[n], self.rs.at[n], dev)
        c.start()
        self.started.append(c)

    def recv(self, n, region):
        remote(region, region, self.ss.at[n], self.rs.at[n], self.p.dev(0, 1)).wait_recv()

    def sibling(self, i, j):
        o = self.p.offs
        self.send(20 + 4 * i + j, self.block(o[i], o[j]), {"ctx": self.p.sib, "tp": self.p.z})

    def item(self, i):
        o = self.p.offs
        if i:
            self.sibling(i, 0)
        self.send(4 + 4 * i, self.block(o[i], 0), self.p.dev(0, 1))
        self.send(5 + 4 * i, self.block(o[i], 0), self.p.dev(0, 3))

    def start(self):
        own = self.block(0, 0)
        self.send(0, own, self.p.dev(1, 0))
        self.send(1, own, self.p.dev(3, 0))
        self.item(0)
        self.sibling(0, 0)

    def first(self):
        self.recv(0, self.block(3, 0))
        self.send(2, self.block(3, 0, 0), self.p.dev(1, 0))
        self.item(1)
        self.recv(1, self.block(1, 0))
        self.send(3, self.block(1, 0, 1), self.p.dev(3, 0))
        self.item(2)

    def second(self):
        self.recv(2, self.block(2, 0, 0))
        self.recv(3, self.block(2, 0, 1))
        self.item(3)

    def third(self, i):
        o = self.p.offs[i]
        self.recv(4 + 4 * i, self.block(o, 3))
        self.send(6 + 4 * i, self.block(o, 3, 0), self.p.dev(0, 1))
        self.sibling(i, 1)
        self.recv(5 + 4 * i, self.block(o, 1))
        self.send(7 + 4 * i, self.block(o, 1, 1), self.p.dev(0, 3))
        self.sibling(i, 2)

    def fourth(self, i):
        o = self.p.offs[i]
        self.recv(6 + 4 * i, self.block(o, 2, 0))
        self.recv(7 + 4 * i, self.block(o, 2, 1))
        self.sibling(i, 3)

    def from_sibling(self, i, j):
        o = self.p.offs
        base = self.p.near(o[i], o[j]) + 1 - 2 * self.p.core
        region = self.buf.at[pl.ds(pl.multiple_of(base * self.rows, 32), self.rows), self.lanes]
        self.recv(20 + 4 * j + i, region)

    def pair_rows(self, i, j):
        o = self.p.offs
        return (self.p.near(o[i], o[j]) - self.p.core) * self.rows

    def finish(self):
        for c in self.started:
            c.wait_send()


class Ring:
    def __init__(self, place, region, ss, rs):
        self.p, self.region, self.ss, self.rs = place, region, ss, rs
        self.started = []

    def copy(self, s, way):
        part = way if s == 4 else None
        src = (s - 1, (NZ + 1 - s) % NZ)[way]
        dst = (s, NZ - s)[way]
        return remote(
            self.region(src, part), self.region(dst, part), self.ss.at[4 * way + s - 1], self.rs.at[4 * way + s - 1],
            {"ctx": self.p.ctx, "tp": (self.p.z + (1, NZ - 1)[way]) % NZ},
        )

    def step(self, s):
        for way in range(2):
            c = self.copy(s, way)
            c.start()
            self.started.append(c)

    def recv(self, s):
        for way in range(2):
            self.copy(s, way).wait_recv()

    def finish(self):
        for c in self.started:
            c.wait_send()


def kernel(
    pat_in, wid_in, pos_in, text_in, cot_in, qkv_in, ow_in, w_in, gain_in,
    normed, grad_out,
    wid, pos, gain, sel, pat, qkv, wf, gf, owf, attf, att_t, att_u, att_v, hacc, perm, colsend, colin, colf, colg, cols, text, cot,
    q0s, q1s, ks, vts, widc, mrow, rows_send, rows_in, incf, idx_send, idx_in, stats, cotsel, scol, drow,
    local, w_ss, w_rs, g_ss, g_rs, ow_ss, ow_rs, osib_ss, osib_rs, at_ss, at_rs,
    ix_ss, ix_rs, rw_ss, rw_rs, co_ss, co_rs, cg_ss, cg_rs, st_ss, st_rs,
):
    p = Place()
    ctx, z, core = p.ctx, p.z, p.core

    def other(d):
        return (ctx + d) % N_CTX

    def behind(d):
        return (ctx + N_CTX - d) % N_CTX

    scope = []

    def mark(name):
        if scope:
            scope.pop().__exit__(None, None, None)
        if name:
            scope.append(jax.named_scope(name))
            scope[-1].__enter__()

    mark("index")
    def block160(ref, c):
        return ref.at[pl.ds(pl.multiple_of(c * ROWS_W, 32), ROWS_W), :]

    barrier = pltpu.get_barrier_semaphore()

    @pl.loop(1, N_CTX)
    def _(d):
        pl.semaphore_signal(barrier, inc=1, device_id={"ctx": other(d), "tp": z}, device_id_type=MESH)

    @pl.loop(1, NZ)
    def _(d):
        pl.semaphore_signal(barrier, inc=1, device_id={"ctx": ctx, "tp": (z + d) % NZ}, device_id_type=MESH)

    load_pos = pltpu.make_async_copy(pos_in, pos, local.at[10])
    load_wid = pltpu.make_async_copy(wid_in, wid, local.at[11])
    load_gain = pltpu.make_async_copy(gain_in, gain, local.at[12])
    load_pos.start()
    load_wid.start()
    load_pat = pltpu.make_async_copy(pat_in, pat, local.at[8])
    load_qkv = pltpu.make_async_copy(qkv_in, qkv, local.at[9])
    load_pat.start()
    load_qkv.start()
    own_w = wf.at[pl.ds(pl.multiple_of(ctx * ROWS_W, 32), ROWS_W), :]
    own_ow = owf.at[pl.ds(0, HCOLS), :]
    load_w = pltpu.make_async_copy(w_in, own_w, local.at[0])
    load_ow = pltpu.make_async_copy(ow_in, own_ow, local.at[1])
    load_text = pltpu.make_async_copy(text_in, text, local.at[2])
    load_cot = pltpu.make_async_copy(cot_in, cot, local.at[3])
    load_w.start()
    load_ow.start()
    load_text.start()
    load_cot.start()
    load_gain.start()
    load_pos.wait()
    load_wid.wait()

    pos_row = pos[...]
    pos_col = jnp.broadcast_to(pos_row, (SLOTS, SLOTS)).T
    t_row = pos_row // TOK
    t_col = pos_col // TOK
    same = t_col == t_row
    earlier_down = same & (iota((SLOTS, SLOTS), 0) < iota((SLOTS, SLOTS), 1))
    earlier_across = same & (iota((SLOTS, SLOTS), 1) < iota((SLOTS, SLOTS), 0))
    rank_row = jnp.sum(jnp.where(earlier_down, 1.0, 0.0).astype(F32), axis=0, keepdims=True)
    rank_col = jnp.sum(jnp.where(earlier_across, 1.0, 0.0).astype(F32), axis=1, keepdims=True)
    live_row = t_row < N_CTX
    bucket_row = jnp.where(live_row, t_row.astype(F32) * 4.0 + rank_row, -1.0)
    to_owner = jnp.where(iota((N_CTX, SLOTS), 0) == t_row, 1.0, 0.0).astype(BF16)
    row_no = pos_col % TOK + 1
    lane_of = rank_col.astype(jnp.int32) * N_CTX + ctx
    at_lane = lane_of == iota((SLOTS, SLOTS), 1)
    high = jnp.where(at_lane, (row_no // 32).astype(F32), 0.0).astype(BF16)
    low = jnp.where(at_lane, (row_no % 32).astype(F32), 0.0).astype(BF16)
    index_rows = (dot(to_owner, high) * 32.0 + dot(to_owner, low)).astype(jnp.int32)
    for t in range(N_CTX):
        idx_send[t] = jnp.broadcast_to(index_rows[t : t + 1, :], (8, SLOTS))
    idx_in[ctx] = idx_send[ctx]

    spread_at = jnp.where(iota((SLOTS, 512), 0) == iota((SLOTS, 512), 1) // 4, 1.0, 0.0).astype(BF16)
    bucket512 = dot(jnp.broadcast_to(bucket_row, (8, SLOTS)).astype(BF16), spread_at)[0:1, :]
    chosen = iota((SLOTS, 512), 0).astype(F32) == bucket512
    for i in range(4):
        sel[i] = jnp.where(chosen & (iota((SLOTS, 512), 1) % 4 == i), 1.0, 0.0).astype(BF16)

    for b in range(4):
        widc[128 * b : 128 * (b + 1), :] = jnp.broadcast_to(wid[:, 128 * b : 128 * (b + 1)], (128, 128)).T

    mark("qkv")
    load_pat.wait()
    load_qkv.wait()
    patches = pat[...]
    lane = iota((512, HCOLS), 1)
    q = dot_nt(patches, qkv[0]).astype(BF16).astype(F32)
    q0s[...] = jnp.where(lane < HEAD_DIM, q, 0.0).astype(BF16)
    q1s[...] = jnp.where(lane < HEAD_DIM, 0.0, q).astype(BF16)
    ks[...] = dot_nt(patches, qkv[1]).astype(BF16)
    vts[...] = dot_nt(qkv[2], patches).astype(BF16)
    mark("barrier")
    pl.semaphore_wait(barrier, N_CTX - 1 + NZ - 1)

    w0, w1 = (PlaneGather(p, wf, ROWS_W, w_ss, w_rs, n) for n in range(2))
    load_w.wait()
    w0.start()
    w1.start()

    def place_of(r):
        return (0, 1, 7, 2, 6, 3, 5, 4).index(r)

    def ow_region(r, part):
        base = pl.multiple_of(place_of(r) * HCOLS + core * 80, 16)
        if part is None:
            return owf.at[pl.ds(base, 80), :]
        return owf.at[pl.ds(base, 80), pl.ds(part * 640, 640)]

    def att_region(r, part):
        if part is None:
            return attf.at[pl.ds(place_of(r) * HCOLS, HCOLS), :]
        return attf.at[pl.ds(place_of(r) * HCOLS + part * 80, 80), :]

    osib = []

    def ow_to_sibling(r):
        src = ow_region(r, None)
        c = remote(src, src, osib_ss.at[r], osib_rs.at[r], {"ctx": p.sib, "tp": z})
        c.start()
        osib.append(c)

    def ow_from_sibling(r):
        dst = owf.at[pl.ds(pl.multiple_of(place_of(r) * HCOLS + (1 - core) * 80, 16), 80), :]
        remote(dst, dst, osib_ss.at[r], osib_rs.at[r], {"ctx": p.sib, "tp": z}).wait_recv()

    og = Ring(p, ow_region, ow_ss, ow_rs)
    ag = Ring(p, att_region, at_ss, at_rs)
    load_ow.wait()
    og.step(1)
    mark("attend")
    factor = 1.0 / HEAD_DIM**0.5

    @pl.loop(0, 4)
    def _(b):
        cols_b = pl.ds(pl.multiple_of(b * 128, 128), 128)
        ids = wid[:, cols_b]
        allowed = (widc[...] == ids) & (widc[...] >= 0)
        parts = []
        for qs in (q0s, q1s):
            scores = dot_nt(ks[...], qs[cols_b, :]) * factor
            scores = jnp.where(allowed, scores, -1e30)
            weights = jnp.exp(scores - jnp.max(scores, axis=0, keepdims=True))
            probs = (weights / jnp.sum(weights, axis=0, keepdims=True)).astype(BF16)
            parts.append(dot(vts[...], probs))
        row = iota((HCOLS, 128), 0)
        attf[0:HCOLS, cols_b] = jnp.where(
            row < HEAD_DIM, parts[0], parts[1]
        ).astype(BF16)

    ag.step(1)

    def turn_att(r):
        k = place_of(r)
        part = attf[k * HCOLS : (k + 1) * HCOLS, :].T
        if k < 5:
            att_t[:, k * HCOLS : (k + 1) * HCOLS] = part
        elif k < 7:
            att_u[:, (k - 5) * HCOLS : (k - 4) * HCOLS] = part
        else:
            att_v[...] = part

    def near_product(n):
        cols_n = slice(n * 256, (n + 1) * 256)
        hacc[:, cols_n] = pat[:, cols_n].astype(F32) + dot(att_t[...], owf[0 : 5 * HCOLS, cols_n])

    def middle_product(n):
        cols_n = slice(n * 256, (n + 1) * 256)
        hacc[:, cols_n] += dot(att_u[:, 0 : 2 * HCOLS], owf[5 * HCOLS : 7 * HCOLS, cols_n])

    turn_att(0)
    mark("w_first0")
    w0.first()
    w0.third(0)
    mark("ow1")
    og.recv(1)
    og.step(2)
    ow_to_sibling(1)
    ow_to_sibling(7)
    mark("w_first1")
    w1.first()
    w1.third(0)
    mark("at1")
    ag.recv(1)
    ag.step(2)
    turn_att(1)
    turn_att(7)

    @pl.loop(1, N_CTX)
    def _(d):
        remote(
            idx_send.at[other(d)], idx_in.at[ctx], ix_ss.at[d], ix_rs.at[d], {"ctx": other(d), "tp": z}
        ).start()

    mark("w_second0")
    w0.second()
    mark("w31_0")
    w0.third(1)
    mark("w_second1")
    w1.second()
    mark("ow2")
    og.recv(2)
    og.step(3)
    ow_to_sibling(2)
    ow_to_sibling(6)
    mark("w32_0")
    w0.third(2)
    mark("w31_1")
    w1.third(1)
    mark("at2")
    ag.recv(2)
    ag.step(3)
    turn_att(2)
    turn_att(6)
    for r in (1, 7, 2, 6):
        ow_from_sibling(r)
    near_product(0)
    mark("w32_1")
    w1.third(2)
    near_product(1)
    mark("w33_0")
    w0.third(3)
    mark("ow3")
    og.recv(3)
    og.step(4)
    ow_to_sibling(3)
    ow_to_sibling(5)
    near_product(2)
    mark("w33_1")
    w1.third(3)
    mark("w40_0")
    w0.fourth(0)
    w0.fourth(1)
    near_product(3)
    mark("at3")
    ag.recv(3)
    ag.step(4)
    turn_att(3)
    turn_att(5)
    mark("w40_1")
    w1.fourth(0)
    w1.fourth(1)
    near_product(4)
    for r in (3, 5):
        ow_from_sibling(r)
    middle_product(0)
    middle_product(1)
    mark("ow4")
    og.recv(4)
    ow_to_sibling(4)
    middle_product(2)
    mark("w42_0")
    w0.fourth(2)
    w0.fourth(3)
    middle_product(3)
    middle_product(4)
    mark("at4")
    ag.recv(4)
    ow_from_sibling(4)
    mark("w42_1")
    w1.fourth(2)
    w1.fourth(3)
    mark("hidden")
    turn_att(4)

    for n in range(5):
        cols_n = slice(n * 256, (n + 1) * 256)
        hidden = (hacc[:, cols_n] + dot(att_v[...], owf[7 * HCOLS : 8 * HCOLS, cols_n])).astype(BF16)
        for i in range(4):
            perm[:, i * DV + n * 256 : i * DV + (n + 1) * 256] = dot(sel[i], hidden).astype(BF16)

    def at_offset(dx, dy, dc):
        x = (ctx // (2 * NY) + dx) % NX
        y = ((ctx // 2) % NY + dy) % NY
        return (x * NY + y) * 2 + (core + dc) % 2

    hops = (0, 1, 2, 1)
    offsets = sorted(
        ((dx, dy, dc) for dx in range(4) for dy in range(4) for dc in range(2) if dx + dy + dc > 0),
        key=lambda o: (-hops[o[0]] - hops[o[1]], o),
    )

    def row_copy(n, part, arriving):
        dx, dy, dc = offsets[n]
        to = at_offset(dx, dy, dc)
        slot = at_offset(-dx % 4, -dy % 4, dc) if arriving else ctx
        lanes = pl.ds(part * 512, 512)
        return remote(
            rows_send.at[to, :, lanes], rows_in.at[slot, :, lanes], rw_ss.at[part, n], rw_rs.at[part, n],
            {"ctx": to, "tp": z},
        )

    for part, w in ((0, w0), (1, w1)):
        mark("w_sib")
        for i in range(4):
            for j in range(4):
                w.from_sibling(i, j)
        mark("merge")
        for n in (2 * part, 2 * part + 1):
            cols_n = slice(256 * n, 256 * (n + 1))
            mrow[:, cols_n] = dot(perm[...], wf[:, cols_n]).astype(BF16).astype(F32)
        lanes = slice(512 * part, 512 * (part + 1))

        @pl.loop(0, N_CTX // 2, unroll=4)
        def _(t):
            eight = mrow[pl.ds(pl.multiple_of(t * 8, 8), 8), lanes]
            rows_send[2 * t, :, lanes] = eight[0:4, :].astype(BF16)
            rows_send[2 * t + 1, :, lanes] = eight[4:8, :].astype(BF16)

        for n in range(len(offsets)):
            row_copy(n, part, False).start()

    rows_in[ctx] = rows_send[ctx]

    mark("colsend")

    def source(zz, x):
        return (x * NY + (x + zz) % NY) * 2 + zz // NY

    x_here = ctx // (2 * NY)
    plane = (z - ((ctx // 2) % NY - x_here + NY) % NY - NY * core + NZ) % NZ
    turn = (plane == 0) | (plane == 2)
    half = plane // 2

    def half_block(c, slot):
        return (
            colsend.at[pl.ds(pl.multiple_of(c * ROWS_W + (half % 2) * 80, 16), 80), :],
            colin.at[pl.ds(pl.multiple_of(slot * 80, 16), 80), :],
        )

    def col_copy(n):
        to = at_offset(*offsets[n])
        slot = (half % 2) * 4 + x_here
        src, dst = half_block(to, slot)
        return remote(src, dst, co_ss.at[n], co_rs.at[slot], {"ctx": to, "tp": z})

    @pl.when(turn)
    def _():
        for n in range(40):
            colsend[n * 128 : (n + 1) * 128, :] = perm[:, n * 128 : (n + 1) * 128].T

        for n in range(len(offsets)):
            col_copy(n).start()
        mine = pl.ds(pl.multiple_of(ctx * ROWS_W + (half % 2) * 80, 16), 80)
        colin[pl.ds(pl.multiple_of(((half % 2) * 4 + x_here) * 80, 16), 80), :] = colsend[mine, :]

    mark("idx_wait")
    @pl.loop(1, N_CTX)
    def _(d):
        remote(
            idx_send.at[other(d)], idx_in.at[behind(d)], ix_ss.at[d], ix_rs.at[d], {"ctx": other(d), "tp": z}
        ).wait()

    mark("cotsel")
    load_text.wait()
    load_cot.wait()
    at_row = (jnp.sum(idx_in[...], axis=0) - 1)[0:1, :]
    at_col = jnp.broadcast_to(at_row, (SLOTS, SLOTS)).T
    for b in range(8):
        drow[:, 128 * b : 128 * (b + 1)] = jnp.where(
            at_col == iota((SLOTS, SLOTS), 1) + 128 * b, 1.0, 0.0
        ).astype(BF16)

    @pl.loop(0, 4)
    def _(n):
        cols_n = pl.ds(pl.multiple_of(n * 256, 256), 256)
        cotsel[:, cols_n] = dot(drow[...], cot[:, cols_n])

    load_gain.wait()
    gains = gain[...].astype(F32)

    def gain_of(n):
        return gains[n : n + 1, :]

    def row_sums(rows, cots):
        sq = jnp.zeros((128, 128), F32)
        inner = jnp.zeros((128, 128), F32)
        for n in range(8):
            cols_n = slice(128 * n, 128 * (n + 1))
            x = rows(cols_n)
            sq = sq + x * x
            inner = inner + x * (gain_of(n) * cots(cols_n))
        return jnp.sum(sq.T, axis=0, keepdims=True), jnp.sum(inner.T, axis=0, keepdims=True)

    mark("text_sums")

    @pl.loop(0, 8)
    def _(b):
        rows_b = pl.ds(pl.multiple_of(b * 128, 128), 128)
        sq, inner = row_sums(
            lambda c: text[rows_b, c].astype(F32), lambda c: cot[rows_b, c].astype(F32)
        )
        stats[z, pl.ds(b, 1), :] = sq
        stats[z, pl.ds(8 + b, 1), :] = inner

    mark("rows_wait")

    for part in range(2):
        for n in range(len(offsets)):
            row_copy(n, part, True).wait()

    mark("embed")

    @pl.loop(0, N_CTX, unroll=4)
    def _(s):
        four = rows_in[s].astype(F32)
        for k in range(4):
            incf[pl.ds(k * N_CTX + s, 1), :] = four[k : k + 1, :]

    mark("new_sums")
    sq_new, inner_new = row_sums(lambda c: incf[:, c], lambda c: cotsel[:, c])
    sq_new = jnp.broadcast_to(sq_new, (SLOTS, SLOTS)).T
    inner_new = jnp.broadcast_to(inner_new, (SLOTS, SLOTS)).T
    for b in range(8):
        here = at_col == iota((SLOTS, SLOTS), 1) + 128 * b
        taken = jnp.sum(jnp.where(here, 1.0, 0.0), axis=0, keepdims=True) > 0.0
        for base, new in ((b, sq_new), (8 + b, inner_new)):
            put = jnp.sum(jnp.where(here, new, 0.0), axis=0, keepdims=True)
            stats[z, base : base + 1, :] = jnp.where(taken, put, stats[z, base : base + 1, :])

    def stat_copy(d, slot):
        return remote(
            stats.at[z], stats.at[slot], st_ss.at[d], st_rs.at[d], {"ctx": ctx, "tp": (z + d) % NZ}
        )

    mark("stat")

    @pl.loop(1, NZ)
    def _(d):
        stat_copy(d, z).start()

    mark("place")
    inc = incf[...].astype(BF16)

    @pl.loop(0, 8)
    def _(b):
        rows_b = pl.ds(pl.multiple_of(b * 128, 128), 128)
        placed = jnp.where(iota((128, SLOTS), 0) + 128 * b == at_row, 1.0, 0.0).astype(F32)
        taken = jnp.sum(placed, axis=1, keepdims=True) > 0.0
        vision = dot(placed.astype(BF16), inc)
        for n in range(8):
            cols_n = slice(128 * n, 128 * (n + 1))
            text[rows_b, cols_n] = jnp.where(taken, vision[:, cols_n].astype(BF16), text[rows_b, cols_n])

    def col_region(r, part):
        if part is None:
            return colin.at[pl.ds(r * 640, 640), :]
        return colin.at[pl.ds(r * 640 + part * 320, 320), :]

    cg = Ring(p, col_region, cg_ss, cg_rs)

    def turn_cols(r):
        @pl.loop(0, 4)
        def _(x):
            for h, ref in ((0, colf), (1, colg)):
                rows_s = pl.ds(pl.multiple_of(source((z + 2 * NZ - r - 2 * h) % NZ, x) * PITCH, 8), SLOTS)
                came = colin[pl.ds(pl.multiple_of(r * 640 + (h * 4 + x) * 80, 16), 80), :].astype(F32)
                ref[rows_s, :] = jnp.concatenate([came, jnp.zeros((48, 128), F32)], axis=0).T

    mark("col_wait")
    for h in range(2):
        for x in range(4):

            @pl.when(ctx != source((z + NZ - 2 * h) % NZ, x))
            def _():
                src, dst = half_block(0, h * 4 + x)
                remote(src, dst, co_ss.at[0], co_rs.at[h * 4 + x], {"ctx": p.sib, "tp": z}).wait_recv()

    cg.step(1)
    mark("stat_wait")

    @pl.loop(1, NZ)
    def _(d):
        stat_copy(d, (z + NZ - d) % NZ).wait()

    mark("drows")
    total = jnp.sum(stats[...], axis=0)
    scale = lax.rsqrt(total[0:8, :] / D + 1e-06)
    inner_all = total[8:16, :]
    scale_at = jnp.zeros((1, SLOTS), F32)
    inner_at = jnp.zeros((1, SLOTS), F32)
    for b in range(8):
        here = iota((128, SLOTS), 0) + 128 * b == at_row
        scale_b = jnp.broadcast_to(scale[b : b + 1, :], (128, 128)).T
        inner_b = jnp.broadcast_to(inner_all[b : b + 1, :], (128, 128)).T
        scol[128 * b : 128 * (b + 1), :] = scale_b
        scale_at = scale_at + jnp.sum(jnp.where(here, scale_b, 0.0), axis=0, keepdims=True)
        inner_at = inner_at + jnp.sum(jnp.where(here, inner_b, 0.0), axis=0, keepdims=True)
    s_at = jnp.broadcast_to(scale_at, (SLOTS, SLOTS)).T
    i_at = jnp.broadcast_to(inner_at, (SLOTS, SLOTS)).T
    own_g = pl.ds(pl.multiple_of(ctx * SLOTS, 128), SLOTS)
    for n in range(8):
        cols_n = slice(128 * n, 128 * (n + 1))
        gained = gain_of(n) * cotsel[:, cols_n]
        gf[own_g, cols_n] = (s_at * gained - incf[:, cols_n] * (s_at * s_at * s_at) * i_at / D).astype(BF16)

    g0, g1 = (PlaneGather(p, gf, SLOTS, g_ss, g_rs, n) for n in range(2))
    g0.start()
    g1.start()

    def normed_block(b):
        for h in range(2):
            rows_b = pl.ds(b * 256 + h * 128, 128)
            for n in range(8):
                cols_n = slice(128 * n, 128 * (n + 1))
                normed[rows_b, cols_n] = (
                    text[rows_b, cols_n].astype(F32) * scol[rows_b, :] * gain_of(n)
                ).astype(BF16)

    def order_block(t):
        for k in range(4):
            rows_k = pl.ds(pl.multiple_of(t * SLOTS + k * N_CTX, 32), N_CTX)
            every = pl.ds(t * 4 + k, N_CTX, stride=PITCH)
            cols[rows_k, 0:80] = colf[every, :][:, 0:80].astype(BF16)
            cols[rows_k, 80:160] = colg[every, :][:, 0:80].astype(BF16)

    def add_pair(i, j, first=False):
        base = g0.pair_rows(i, j)
        rows_p = pl.ds(pl.multiple_of(base, 256), 256)
        part = lax.dot_general(
            cols[rows_p, :], gf[rows_p, :], (((0,), (0,)), ((), ())), preferred_element_type=F32
        )
        grad_out[...] = part if first else grad_out[...] + part

    def pair(i, j, first=False):
        base = g0.pair_rows(i, j) // SLOTS
        for h in range(2):
            order_block(base + h)
        g0.from_sibling(i, j)
        g1.from_sibling(i, j)
        add_pair(i, j, first)

    mark("normed")
    normed_block(0)
    normed_block(1)
    normed_block(2)
    normed_block(3)
    turn_cols(0)
    mark("c1")
    cg.recv(1)
    cg.step(2)
    mark("g1_0")
    g0.first()
    g0.third(0)
    mark("col_t")
    turn_cols(1)
    turn_cols(7)
    mark("g1_1")
    g1.first()
    g1.third(0)
    mark("c2")
    cg.recv(2)
    cg.step(3)
    mark("g2_0")
    g0.second()
    mark("g31_0")
    g0.third(1)
    mark("col_t")
    turn_cols(2)
    turn_cols(6)
    mark("g2_1")
    g1.second()
    mark("g32_0")
    g0.third(2)
    mark("g31_1")
    g1.third(1)
    mark("c3")
    cg.recv(3)
    cg.step(4)
    mark("col_t")
    turn_cols(3)
    turn_cols(5)
    mark("g32_1")
    g1.third(2)
    mark("g33_0")
    g0.third(3)
    mark("c4")
    cg.recv(4)
    mark("g33_1")
    g1.third(3)
    mark("col_t")
    turn_cols(4)
    mark("add0")
    pair(0, 0, True)
    pair(1, 0)
    pair(0, 1)
    mark("g40_0")
    g0.fourth(0)
    g0.fourth(1)
    mark("add1")
    pair(2, 0)
    pair(0, 2)
    pair(1, 1)
    mark("g40_1")
    g1.fourth(0)
    g1.fourth(1)
    mark("add2")
    pair(1, 2)
    pair(2, 1)
    pair(2, 2)
    mark("g42_0")
    g0.fourth(2)
    mark("add3")
    pair(3, 0)
    pair(0, 3)
    mark("g42_1")
    g1.fourth(2)
    mark("g43_0")
    g0.fourth(3)
    mark("add4")
    pair(3, 1)
    pair(1, 3)
    mark("g43_1")
    g1.fourth(3)
    mark("add5")
    pair(3, 2)
    pair(2, 3)
    pair(3, 3)
    mark("end")
    for c in (w0, w1, g0, g1, og, ag, cg):
        c.finish()
    for c in osib:
        c.wait_send()

    @pl.when(turn)
    def _():
        for n in range(len(offsets)):
            col_copy(n).wait_send()

    mark(None)


def hand_out(normed, grad, normed_out, grad_out, sems):
    go = [
        pltpu.make_async_copy(normed.at[pl.ds(r, 256), :], normed_out.at[pl.ds(r, 256), :], sems.at[r // 256])
        for r in range(0, TOK, 256)
    ] + [pltpu.make_async_copy(grad, grad_out, sems.at[4])]
    for g in go:
        g.start()
    for g in go:
        g.wait()


def shards(
    patches,
    window_ids,
    positions,
    text_embed,
    cotangent,
    qkv_weight,
    out_weight,
    merger_weight,
    norm_gain,
):
    vmem = pl.BlockSpec(memory_space=pltpu.VMEM)
    anywhere = pl.BlockSpec(memory_space=pl.ANY)
    dma = pltpu.SemaphoreType.DMA
    outs = pl.pallas_call(
        kernel,
        out_shape=(pltpu.VMEM((TOK, 1024), BF16), pltpu.VMEM((ROWS_W, 1024), F32)),
        in_specs=[anywhere] * 9,
        out_specs=(vmem, vmem),
        scratch_shapes=[
            pltpu.VMEM((1, 512), jnp.int32),
            pltpu.VMEM((1, SLOTS), jnp.int32),
            pltpu.VMEM((8, 128), BF16),
            pltpu.VMEM((4, SLOTS, 512), BF16),
            pltpu.VMEM((512, DV), BF16),
            pltpu.VMEM((3, HCOLS, DV), BF16),
            pltpu.VMEM((N_CTX * ROWS_W, 1024), BF16),
            pltpu.VMEM((N_CTX * SLOTS, 1024), BF16),
            pltpu.VMEM((DV, DV), BF16),
            pltpu.VMEM((DV, 512), BF16),
            pltpu.VMEM((512, 5 * HCOLS), BF16),
            pltpu.VMEM((512, 2 * HCOLS), BF16),
            pltpu.VMEM((512, HCOLS), BF16),
            pltpu.VMEM((512, DV), F32),
            pltpu.VMEM((SLOTS, 4 * DV), BF16),
            pltpu.VMEM((4 * DV, SLOTS), BF16),
            pltpu.VMEM((N_CTX * ROWS_W, SLOTS), BF16),
            pltpu.VMEM((N_CTX * PITCH, 128), F32),
            pltpu.VMEM((N_CTX * PITCH, 128), F32),
            pltpu.VMEM((N_CTX * SLOTS, ROWS_W), BF16),
            pltpu.VMEM((TOK, 1024), BF16),
            pltpu.VMEM((TOK, 1024), BF16),
            pltpu.VMEM((512, HCOLS), BF16),
            pltpu.VMEM((512, HCOLS), BF16),
            pltpu.VMEM((512, HCOLS), BF16),
            pltpu.VMEM((HCOLS, 512), BF16),
            pltpu.VMEM((512, 128), jnp.int32),
            pltpu.VMEM((SLOTS, 1024), F32),
            pltpu.VMEM((N_CTX, 4, 1024), BF16),
            pltpu.VMEM((N_CTX, 4, 1024), BF16),
            pltpu.VMEM((SLOTS, 1024), F32),
            pltpu.VMEM((N_CTX, 8, SLOTS), jnp.int32),
            pltpu.VMEM((N_CTX, 8, SLOTS), jnp.int32),
            pltpu.VMEM((NZ, 16, SLOTS), F32),
            pltpu.VMEM((SLOTS, 1024), F32),
            pltpu.VMEM((TOK, SLOTS), F32),
            pltpu.VMEM((SLOTS, TOK), BF16),
            dma((13,)),
            dma((2, 36)), dma((2, 36)), dma((2, 36)), dma((2, 36)),
            dma((8,)), dma((8,)), dma((8,)), dma((8,)), dma((8,)), dma((8,)),
            dma((N_CTX,)), dma((N_CTX,)), dma((2, N_CTX)), dma((2, N_CTX)), dma((N_CTX,)), dma((8,)), dma((8,)), dma((8,)),
            dma((NZ,)), dma((NZ,)),
        ],
        compiler_params=pltpu.CompilerParams(
            collective_id=0, has_side_effects=True, vmem_limit_bytes=56 * 1024 * 1024
        ),
    )(
        patches,
        window_ids.reshape(1, -1),
        positions.reshape(1, -1),
        text_embed,
        cotangent,
        jnp.swapaxes(qkv_weight, 1, 2),
        out_weight,
        merger_weight,
        norm_gain.reshape(8, 128),
    )
    return pl.pallas_call(
        hand_out,
        out_shape=(
            jax.ShapeDtypeStruct((TOK, 1024), BF16),
            jax.ShapeDtypeStruct((ROWS_W, 1024), F32),
        ),
        in_specs=[anywhere, anywhere],
        out_specs=(anywhere, anywhere),
        scratch_shapes=[
            dma((5,)),
        ],
        compiler_params=pltpu.CompilerParams(vmem_limit_bytes=1024 * 1024),
    )(*outs)


def solution(mesh):
    in_specs = (
        P("ctx", None),
        P("ctx"),
        P("ctx"),
        P("ctx", "tp"),
        P("ctx", "tp"),
        P(None, None, "tp"),
        P("tp", None),
        P("ctx", "tp"),
        P("tp"),
    )
    out_specs = (P("ctx", "tp"), P("ctx", "tp"))
    return jax.shard_map(shards, mesh=mesh, in_specs=in_specs, out_specs=out_specs, check_vma=False)
```
